32 devices in a mesh: case: 2 (over x), model: 4 (over z), ens: 4 (over y, core).
Axes of the slice: x: 2, y: 2, z: 4, core: 2. Of those that a mesh axis runs over, the one named last changes fastest.
Arguments:
- ens_init: float32 [64, 2048, 48], P(('case', 'ens'), None, 'model'), parts along dimension 0
- mix_op: bfloat16 [2048, 2048], replicated
- w_in: bfloat16 [3, 48, 768], P(None, None, 'model')
- w_out: bfloat16 [3, 768, 48], P(None, 'model')
- obs_val: float32 [3, 4096, 12], P(None, ('case', 'ens', 'model')), parts along dimension 1
- obs_prec: float32 [4096, 12], P(('case', 'ens', 'model')), parts along dimension 0
- obs_idx: int32 [12], replicated
- inflation: float32 [1], replicated
Outputs:
- output: float32 [64, 2048, 48], P(('case', 'ens'), None, 'model'), parts along dimension 0
There are 2 independent parts. The reference program is written for one: setup_inputs(seed, part) draws one part's arguments, and reference() takes and returns one part's arrays. A program takes and returns all parts, laid end to end along the dimension named above; an argument that names none is the same for every part.
All inputs are finite; a program needn't handle non-finite values.
Results may differ from the reference program's by a relative error of at most 0.0173175.
Values are sent between devices in bfloat16 or wider.
A program may use at most 1 GiB of HBM per device.

```python
import jax
import jax.numpy as jnp
from jax import lax

COLS = 2048
VARS = 48
HIDDEN = 768
OBS_VARS = 12
LAYERS = 3
CYCLES = 3
MEMBERS = 32
NS_STEPS = 12
COL_BLOCK = 128


def setup_inputs(seed: int = 0, part: int = 0) -> dict:
    shared_keys = jax.random.split(jax.random.key(seed), 5)
    part_keys = jax.random.split(jax.random.fold_in(jax.random.key(seed + 1), part), 4)
    base_state = jax.random.normal(part_keys[0], (COLS, VARS), jnp.float32)
    spread = jax.random.normal(part_keys[1], (MEMBERS, COLS, VARS), jnp.float32)
    ens_init = base_state[None] + 0.4 * spread
    obs_val = jax.random.normal(part_keys[2], (CYCLES, COLS, OBS_VARS), jnp.float32)
    obs_prec = jax.random.uniform(part_keys[3], (COLS, OBS_VARS), jnp.float32, 0.75, 5.25)
    mix_op = (jax.random.normal(shared_keys[0], (COLS, COLS), jnp.float32) * COLS ** -0.5).astype(jnp.bfloat16)
    w_in = (jax.random.normal(shared_keys[1], (LAYERS, VARS, HIDDEN), jnp.float32) * VARS ** -0.5).astype(jnp.bfloat16)
    w_out = (jax.random.normal(shared_keys[2], (LAYERS, HIDDEN, VARS), jnp.float32) * (0.5 * HIDDEN ** -0.5)).astype(jnp.bfloat16)
    obs_idx = jax.random.permutation(shared_keys[3], VARS)[:OBS_VARS].astype(jnp.int32)
    inflation = jax.random.uniform(shared_keys[4], (1,), jnp.float32, 1.0, 1.6)
    return dict(ens_init=ens_init, mix_op=mix_op, w_in=w_in, w_out=w_out, obs_val=obs_val, obs_prec=obs_prec, obs_idx=obs_idx, inflation=inflation)


def forecast_member(member, mix_op, w_in, w_out):
    def layer_step(state_now, weights):
        w_first, w_second = weights
        mix_out = jnp.dot(mix_op, state_now.astype(jnp.bfloat16), preferred_element_type=jnp.float32).astype(jnp.bfloat16)
        hidden = jax.nn.gelu(jnp.dot(mix_out, w_first, preferred_element_type=jnp.float32), approximate=True)
        update = jnp.dot(hidden.astype(jnp.bfloat16), w_second, preferred_element_type=jnp.float32)
        return state_now + update, None
    result, unused = lax.scan(layer_step, member, (w_in, w_out))
    return result


def analyse_block(col_block, obs_now, prec_now, obs_idx, inflation):
    ens_mean = jnp.mean(col_block, axis=1)
    anomaly = col_block - ens_mean[:, None, :]
    obs_anom = jnp.take(anomaly, obs_idx, axis=2)
    innovation = obs_now - jnp.take(ens_mean, obs_idx, axis=1)
    weighted = obs_anom * prec_now[:, None, :]
    identity = jnp.eye(MEMBERS, dtype=jnp.float32)
    a_tilde = ((MEMBERS - 1) / inflation[0]) * identity + jnp.einsum('bip,bjp->bij', weighted, obs_anom)
    trace_sum = jnp.trace(a_tilde, axis1=1, axis2=2)[:, None, None]
    b_mat = a_tilde / trace_sum
    z_mat = jnp.broadcast_to(identity, a_tilde.shape)
    for ns_step in range(NS_STEPS):
        t_mat = 1.5 * identity - 0.5 * jnp.einsum('bij,bjk->bik', z_mat, b_mat)
        b_mat = jnp.einsum('bij,bjk->bik', b_mat, t_mat)
        z_mat = jnp.einsum('bij,bjk->bik', t_mat, z_mat)
    sqrt_inv = z_mat / jnp.sqrt(trace_sum)
    gain_vec = jnp.einsum('bip,bp->bi', weighted, innovation)
    half_step = jnp.einsum('bij,bj->bi', sqrt_inv, gain_vec)
    w_mean = jnp.einsum('bij,bj->bi', sqrt_inv, half_step)
    w_full = (MEMBERS - 1) ** 0.5 * sqrt_inv + w_mean[:, :, None]
    return ens_mean[:, None, :] + jnp.einsum('bik,biv->bkv', w_full, anomaly)


def reference(ens_init, mix_op, w_in, w_out, obs_val, obs_prec, obs_idx, inflation):
    n_blocks = COLS // COL_BLOCK
    prec_blocks = obs_prec.reshape(n_blocks, COL_BLOCK, OBS_VARS)

    def forecast_one(member):
        return forecast_member(member, mix_op, w_in, w_out)

    def analyse_pieces(pieces):
        return analyse_block(pieces[0], pieces[1], pieces[2], obs_idx, inflation)

    def run_cycle(ens_state, obs_now):
        ens_state = lax.map(forecast_one, ens_state)
        col_blocks = ens_state.reshape(MEMBERS, n_blocks, COL_BLOCK, VARS).transpose(1, 2, 0, 3)
        obs_blocks = obs_now.reshape(n_blocks, COL_BLOCK, OBS_VARS)
        analysed = lax.map(analyse_pieces, (col_blocks, obs_blocks, prec_blocks))
        return analysed.transpose(2, 0, 1, 3).reshape(MEMBERS, COLS, VARS), None

    final_state, unused = lax.scan(run_cycle, ens_init, obs_val)
    return final_state
```

```python
import functools

import jax
import jax.numpy as jnp
from jax import lax
from jax.experimental import pallas as pl
from jax.experimental.pallas import tpu as pltpu
from jax.sharding import PartitionSpec as P

NS_STEPS = 12
MESH_IDS = pl.DeviceIdType.MESH
F32 = jnp.float32
BF16 = jnp.bfloat16
C1 = 0.7978845608028654
C2 = 0.7978845608028654 * 0.044715


def gelu(x):
    th = jnp.tanh(x * (C1 + C2 * (x * x)))
    half = 0.5 * x
    return half + half * th


def kernel(dims, idx_ref, rho_ref, x0_ref, a_hbm, wu_ref, y_ref, r_ref, out_ref,
           a_v, at, wu_all, wt, ut, s0, r0, hw, hb, mt, recv_c, recv_f, send_f, out_s, out_r,
           v_s, f_s, ft_s, m_s, c_m, dn_m, dz_m, t_m, q_m,
           sem_a, sem_ws, sem_wr, sem_is, sem_ir, sem_cs, sem_cr, sem_fs, sem_fr, sem_os, sem_or):
    cycles, layers, n_obs = dims
    me_e = lax.axis_index("ens")
    me_m = lax.axis_index("model")
    me = me_e * 4 + me_m
    my_half = me_m // 2
    members = 32

    def ids(te, tm):
        return {"ens": te, "model": tm}

    bar = pltpu.get_barrier_semaphore()
    for de in range(4):
        for dm in range(4):
            if (de, dm) != (0, 0):
                pl.semaphore_signal(bar, inc=1, device_id=ids((me_e + de) % 4, (me_m + dm) % 4), device_id_type=MESH_IDS)
    copy_a = pltpu.make_async_copy(a_hbm, a_v, sem_a)
    copy_a.start()

    for j in range(16):
        out_s[j] = x0_ref[:, j * 128:(j + 1) * 128]
        for a in range(2):
            for d in range(4):
                s0[a, d, :, j * 128:(j + 1) * 128] = out_s[j, pl.ds(2 * d + a, 12, stride=8), :]
    pl.semaphore_wait(bar, 15)

    def init_copy(a, dm):
        tm = (me_m + dm) % 4
        return pltpu.make_async_remote_copy(
            src_ref=s0.at[a, tm], dst_ref=r0.at[a, me_m], send_sem=sem_is.at[a, tm], recv_sem=sem_ir.at[a, me_m],
            device_id=ids(me_e, tm), device_id_type=MESH_IDS)

    def init_wait(a, dm):
        tm = (me_m + dm) % 4
        return pltpu.make_async_remote_copy(
            src_ref=s0.at[a, tm], dst_ref=r0.at[a, tm], send_sem=sem_is.at[a, tm], recv_sem=sem_ir.at[a, tm],
            device_id=ids(me_e, tm), device_id_type=MESH_IDS)

    def w_copy(dm):
        tm = (me_m + dm) % 4
        return pltpu.make_async_remote_copy(
            src_ref=wu_ref, dst_ref=wu_all.at[me_m], send_sem=sem_ws.at[tm], recv_sem=sem_wr.at[me_m],
            device_id=ids(me_e, tm), device_id_type=MESH_IDS)

    def w_wait(dm):
        tm = (me_m + dm) % 4
        return pltpu.make_async_remote_copy(
            src_ref=wu_ref, dst_ref=wu_all.at[tm], send_sem=sem_ws.at[tm], recv_sem=sem_wr.at[tm],
            device_id=ids(me_e, tm), device_id_type=MESH_IDS)

    for dm in (2, 1, 3):
        init_copy(0, dm).start()
    for dm in (2, 1, 3):
        w_copy(dm).start()
    for dm in (2, 1, 3):
        init_copy(1, dm).start()
    for a in range(2):
        r0[a, me_m] = s0[a, me_m]
    wu_all[me_m] = wu_ref[...]
    mt[48:128, :] = jnp.zeros((80, 2048), BF16)

    copy_a.wait()
    row = lax.broadcasted_iota(jnp.int32, (256, 256), 0)
    col = lax.broadcasted_iota(jnp.int32, (256, 256), 1)
    eye = jnp.where(row == col, 1.0, 0.0).astype(BF16)

    def flip(i, carry):
        for j in range(8):
            tile = a_v[pl.ds(pl.multiple_of(i * 256, 256), 256), j * 256:(j + 1) * 256]
            at[j * 256:(j + 1) * 256, pl.ds(pl.multiple_of(i * 256, 256), 256)] = lax.dot_general(
                eye, tile, (((1,), (1,)), ((), ())), preferred_element_type=F32).astype(BF16)
        return carry

    lax.fori_loop(0, 8, flip, 0)

    for dm in (2, 1, 3):
        w_wait(dm).wait()
    lane = lax.broadcasted_iota(jnp.int32, (192, 128), 1)
    for l in range(layers):
        parts = []
        for q in range(4):
            piece = wu_all[q, l].astype(F32)
            wt[l, q * 192:(q + 1) * 192, :] = jnp.where(lane < 48, piece, 0.0).astype(BF16)
            parts.append(piece)
        ut[l] = jnp.transpose(jnp.concatenate(parts, axis=0))[64:112, :].astype(BF16)

    def pick(i):
        half = (my_half + 1 - i // 8) % 2
        te = (me_e + (i % 8) // 2) % 4
        tm = 2 * half + i % 2
        return te, tm, te * 4 + tm

    def c_copy(a, te, tm, slot):
        t = te * 4 + tm
        return pltpu.make_async_remote_copy(
            src_ref=hw.at[a, :, pl.ds(pl.multiple_of(t * 128, 128), 128)], dst_ref=recv_c.at[slot, a],
            send_sem=sem_cs.at[a, t], recv_sem=sem_cr.at[a, slot], device_id=ids(te, tm), device_id_type=MESH_IDS)

    def f_copy(a, te, tm, slot):
        t = te * 4 + tm
        return pltpu.make_async_remote_copy(
            src_ref=send_f.at[a, t], dst_ref=recv_f.at[a, slot],
            send_sem=sem_fs.at[a, t], recv_sem=sem_fr.at[a, slot], device_id=ids(te, tm), device_id_type=MESH_IDS)

    def o_copy(te, tm, slot):
        t = te * 4 + tm
        return pltpu.make_async_remote_copy(
            src_ref=out_s.at[t], dst_ref=out_r.at[:, pl.ds(pl.multiple_of(slot * 128, 128), 128)],
            send_sem=sem_os.at[t], recv_sem=sem_or.at[slot], device_id=ids(te, tm), device_id_type=MESH_IDS)

    def others(fn):
        def body(i, carry):
            te, tm, t = pick(i)

            @pl.when(t != me)
            def _():
                fn(te, tm, t)
            return carry
        lax.fori_loop(0, 16, body, 0)

    def forecast(cyc, a):
        @pl.when(cyc == 0)
        def _():
            for dm in (2, 1, 3):
                init_wait(a, dm).wait()
            for q in range(4):
                hw[a, q * 12:(q + 1) * 12, :] = r0[a, q]
            hb[...] = hw[a].astype(BF16)

        @pl.when(cyc > 0)
        def _():
            def drain(te, tm, t):
                c_copy(a, te, tm, t).wait_send()
                f_copy(a, te, tm, t).wait()
            others(drain)

            def load(j, carry):
                sl = pl.ds(pl.multiple_of(j * 128, 128), 128)
                block = recv_f[a, j]
                hw[a, :, sl] = block
                hb[:, sl] = block.astype(BF16)
                return carry
            lax.fori_loop(0, 16, load, 0)

        def layer(l, carry):
            for n in range(4):
                mt[0:48, n * 512:(n + 1) * 512] = jnp.dot(
                    hb[...], at[:, n * 512:(n + 1) * 512], preferred_element_type=F32).astype(BF16)

            def tile(i, inner):
                half = (my_half + 1 - i // 4) % 2
                te = (me_e + i % 4) % 4
                sl = pl.ds(pl.multiple_of((2 * te + half) * 256, 256), 256)
                mix = mt[:, sl]
                new = hw[a, :, sl]
                upd = None
                for n in range(3):
                    hid = jnp.dot(wt[l, n * 256:(n + 1) * 256, :], mix, preferred_element_type=F32)
                    part = jnp.dot(ut[l, :, n * 256:(n + 1) * 256], gelu(hid).astype(BF16), preferred_element_type=F32)
                    upd = part if upd is None else upd + part
                new = new + upd
                hw[a, :, sl] = new
                hb[:, sl] = new.astype(BF16)

                @pl.when(l == layers - 1)
                def _():
                    for b in range(2):
                        tm = 2 * half + b
                        t = te * 4 + tm

                        @pl.when(t != me)
                        def _():
                            c_copy(a, te, tm, me).start()

                        @pl.when(t == me)
                        def _():
                            recv_c[me, a] = new[:, b * 128:(b + 1) * 128]
                return inner
            lax.fori_loop(0, 8, tile, 0)
            return carry
        lax.fori_loop(0, layers, layer, 0)

    def mat(p_ref, rows):
        out = []
        for i in range(n_obs):
            acc = None
            for k in range(n_obs):
                term = p_ref[i, k:k + 1, :] * rows[k]
                acc = term if acc is None else acc + term
            out.append(acc)
        return out

    def vec(p_ref, x):
        acc = None
        for k in range(n_obs):
            term = x[k:k + 1, :] * p_ref[k]
            acc = term if acc is None else acc + term
        return acc

    sub = lax.broadcasted_iota(jnp.int32, (n_obs, 128), 0)
    units = [jnp.where(sub == i, 1.0, 0.0).astype(F32) for i in range(n_obs)]
    c0 = (members - 1) / rho_ref[0]

    def analyse(cyc):
        for a in range(2):
            others(lambda te, tm, t: c_copy(a, te, tm, t).wait_recv())

        def add(j, acc):
            return acc + (recv_c[j, 0] + recv_c[j, 1])
        mean = lax.fori_loop(0, 16, add, jnp.zeros((48, 128), F32)) * (1.0 / members)
        m_s[...] = mean

        def centre(j, carry):
            for a in range(2):
                recv_c[j, a] = recv_c[j, a] - mean
            return carry
        lax.fori_loop(0, 16, centre, 0)

        root = jnp.sqrt(r_ref[...])
        for p in range(n_obs):
            ip = idx_ref[p]
            v_s[:, :, p:p + 1, :] = recv_c[:, :, pl.ds(ip, 1), :] * root[p:p + 1, :]

        for grp in range(0, n_obs, 6):
            def outer(j, accs):
                accs = list(accs)
                for a in range(2):
                    x = recv_c[j, a]
                    for p in range(6):
                        accs[p] = accs[p] + v_s[j, a, grp + p:grp + p + 1, :] * x
                return tuple(accs)
            sums = lax.fori_loop(0, 16, outer, tuple(jnp.zeros((48, 128), F32) for _ in range(6)))
            for p in range(6):
                f_s[grp + p] = sums[p]

        gain = []
        for q in range(n_obs):
            iq = idx_ref[q]
            c_m[:, q:q + 1, :] = f_s[:, pl.ds(iq, 1), :] * root[q:q + 1, :]
            gain.append(root[q:q + 1, :] * (y_ref[cyc, q:q + 1, :] - m_s[pl.ds(iq, 1), :]))
        gain = jnp.concatenate(gain, axis=0)

        trace = None
        for p in range(n_obs):
            term = c_m[p, p:p + 1, :]
            trace = term if trace is None else trace + term
        trace = trace + members * c0
        inv = 1.0 / trace
        for p in range(n_obs):
            dn_m[p] = units[p] * inv
            dz_m[p] = jnp.zeros((n_obs, 128), F32)

        def step(i, carry):
            n, z = carry
            t = 1.5 - 0.5 * n
            c_rows = [c_m[k] for k in range(n_obs)]
            nc = mat(dn_m, c_rows)
            for p in range(n_obs):
                t_m[p] = t * units[p] - 0.5 * nc[p]
            tz = mat(t_m, [dz_m[k] for k in range(n_obs)])
            tt = mat(t_m, [t_m[k] for k in range(n_obs)])
            for p in range(n_obs):
                dz_m[p] = tz[p] - (0.5 * z) * dn_m[p]
                q_m[p] = tt[p] - (0.5 * n) * (t_m[p] + t * units[p])
            dn = mat(dn_m, [q_m[k] for k in range(n_obs)])
            for p in range(n_obs):
                dn_m[p] = dn[p]
            return n * t * t, t * z
        n, z = lax.fori_loop(0, NS_STEPS, step, (c0 * inv, jnp.ones((1, 128), F32)))

        rs = 1.0 / jnp.sqrt(trace)
        scale = float((members - 1) ** 0.5) * rs
        alpha = scale * z

        def apply_z(x):
            return z * x + vec(dz_m, vec(c_m, x))
        h = apply_z(apply_z(gain)) * inv

        base = m_s[...]
        for p in range(n_obs):
            base = base + h[p:p + 1, :] * f_s[p]
        m_s[...] = base
        for q in range(n_obs):
            acc = None
            for p in range(n_obs):
                term = (scale * dz_m[q, p:p + 1, :]) * f_s[p]
                acc = term if acc is None else acc + term
            ft_s[q] = acc

        def updated(t, a):
            acc = m_s[...] + alpha * recv_c[t, a]
            for q in range(n_obs):
                acc = acc + v_s[t, a, q:q + 1, :] * ft_s[q]
            return acc

        @pl.when(cyc < cycles - 1)
        def _():
            for a in range(2):
                def back(i, carry):
                    te, tm, t = pick(i)
                    new = updated(t, a)

                    @pl.when(t != me)
                    def _():
                        send_f[a, t] = new
                        f_copy(a, te, tm, me).start()

                    @pl.when(t == me)
                    def _():
                        recv_f[a, me] = new
                    return carry
                lax.fori_loop(0, 16, back, 0)

        @pl.when(cyc == cycles - 1)
        def _():
            def final(i, carry):
                te = (me_e + i) % 4
                for k in range(8):
                    new = updated(te * 4 + k // 2, k % 2)
                    for q in range(4):
                        out_s[te * 4 + q, pl.ds(k, 12, stride=8), :] = new[q * 12:(q + 1) * 12, :]
                for dm in (2, 1, 3, 0):
                    tm = (me_m + dm) % 4
                    t = te * 4 + tm

                    @pl.when(t != me)
                    def _():
                        o_copy(te, tm, me).start()

                    @pl.when(t == me)
                    def _():
                        out_r[:, pl.ds(pl.multiple_of(me * 128, 128), 128)] = out_s[me]
                return carry
            lax.fori_loop(0, 4, final, 0)

    def cycle(cyc, carry):
        forecast(cyc, 0)
        forecast(cyc, 1)
        analyse(cyc)
        return carry
    lax.fori_loop(0, cycles, cycle, 0)

    def finish(te, tm, t):
        for a in range(2):
            c_copy(a, te, tm, t).wait_send()
        o_copy(te, tm, t).wait()
    others(finish)
    out_ref[...] = out_r[...]


def solution(mesh):
    def local_step(ens_local, mix_op, w_in, w_out, obs_val, obs_prec, obs_idx, inflation):
        cycles, layers = obs_val.shape[0], w_in.shape[0]
        n_obs = obs_idx.shape[0]
        x0 = jnp.transpose(ens_local, (2, 0, 1)).reshape(96, 2048)
        zero = jnp.zeros((layers, 192, 16), BF16)
        wu = jnp.concatenate([jnp.transpose(w_in, (0, 2, 1)), zero, w_out, zero], axis=2)
        yobs = jnp.transpose(obs_val, (0, 2, 1))
        rinv = jnp.transpose(obs_prec)
        vmem = pl.BlockSpec(memory_space=pltpu.VMEM)
        smem = pl.BlockSpec(memory_space=pltpu.SMEM)
        dma = pltpu.SemaphoreType.DMA
        out = pl.pallas_call(
            functools.partial(kernel, (cycles, layers, n_obs)),
            out_shape=jax.ShapeDtypeStruct((96, 2048), F32),
            in_specs=[smem, smem, vmem, pl.BlockSpec(memory_space=pl.ANY), vmem, vmem, vmem],
            out_specs=vmem,
            scratch_shapes=[
                pltpu.VMEM((2048, 2048), BF16),
                pltpu.VMEM((2048, 2048), BF16),
                pltpu.VMEM((4, layers, 192, 128), BF16),
                pltpu.VMEM((layers, 768, 128), BF16),
                pltpu.VMEM((layers, 48, 768), BF16),
                pltpu.VMEM((2, 4, 12, 2048), F32),
                pltpu.VMEM((2, 4, 12, 2048), F32),
                pltpu.VMEM((2, 48, 2048), F32),
                pltpu.VMEM((48, 2048), BF16),
                pltpu.VMEM((128, 2048), BF16),
                pltpu.VMEM((16, 2, 48, 128), F32),
                pltpu.VMEM((2, 16, 48, 128), F32),
                pltpu.VMEM((2, 16, 48, 128), F32),
                pltpu.VMEM((16, 96, 128), F32),
                pltpu.VMEM((96, 2048), F32),
                pltpu.VMEM((16, 2, n_obs, 128), F32),
                pltpu.VMEM((n_obs, 48, 128), F32),
                pltpu.VMEM((n_obs, 48, 128), F32),
                pltpu.VMEM((48, 128), F32),
                pltpu.VMEM((n_obs, n_obs, 128), F32),
                pltpu.VMEM((n_obs, n_obs, 128), F32),
                pltpu.VMEM((n_obs, n_obs, 128), F32),
                pltpu.VMEM((n_obs, n_obs, 128), F32),
                pltpu.VMEM((n_obs, n_obs, 128), F32),
                dma(()),
                dma((4,)), dma((4,)),
                dma((2, 4)), dma((2, 4)),
                dma((2, 16)), dma((2, 16)),
                dma((2, 16)), dma((2, 16)),
                dma((16,)), dma((16,)),
            ],
            compiler_params=pltpu.CompilerParams(
                collective_id=0, has_side_effects=True, vmem_limit_bytes=60 * 1024 * 1024),
        )(obs_idx, inflation, x0, mix_op, wu, yobs, rinv)
        return jnp.transpose(out.reshape(12, 8, 2048), (1, 2, 0))

    member_spec = P(("case", "ens"), None, "model")
    col_axes = ("case", "ens", "model")
    in_specs = (member_spec, P(None, None), P(None, None, "model"), P(None, "model", None), P(None, col_axes, None), P(col_axes, None), P(None), P(None))
    return jax.shard_map(local_step, mesh=mesh, in_specs=in_specs, out_specs=member_spec, check_vma=False)
```

```python
import functools

import jax
import jax.numpy as jnp
from jax import lax
from jax.experimental import pallas as pl
from jax.experimental.pallas import tpu as pltpu
from jax.sharding import PartitionSpec as P

NS_STEPS = 12
MESH_IDS = pl.DeviceIdType.MESH
F32 = jnp.float32
BF16 = jnp.bfloat16
C1 = 0.7978845608028654
C2 = 0.7978845608028654 * 0.044715


def gelu(x):
    th = jnp.tanh(x * (C1 + C2 * (x * x)))
    half = 0.5 * x
    return half + half * th


def kernel(dims, idx_ref, rho_ref, x0_ref, a_hbm, w_ref, u_ref, y_in, r_in, out_ref,
           a_v, at, wall, wt, ut, s0, r0, relay, y_ref, r_ref, hw, hb, recv_c, recv_f, send_f, out_s, out_r,
           v_s, f_s, ft_s, m_s, c_m, dn_m, dz_m, t_m, q_m,
           sem_a, sem_ws, sem_wr, sem_ds, sem_dr, sem_bs, sem_br, sem_is, sem_ir, sem_rs, sem_rr,
           sem_cs, sem_cr, sem_fs, sem_fr, sem_os, sem_or):
    cycles, layers, n_obs = dims
    me_x = lax.axis_index("case")
    me_e = lax.axis_index("ens")
    me_z = lax.axis_index("model")
    grp = me_z // 2
    low = me_z % 2
    core = me_e % 2
    far = 1 - me_x
    mate = me_e + 1 - 2 * core
    me = me_e * 4 + me_x * 2 + low
    inside = grp == me_x
    members = 32

    def ids(tx, te, tz):
        return {"case": tx, "ens": te, "model": tz}

    def send(src, dst, ssem, rsem, dev):
        return pltpu.make_async_remote_copy(
            src_ref=src, dst_ref=dst, send_sem=ssem, recv_sem=rsem, device_id=dev, device_id_type=MESH_IDS)

    bar = pltpu.get_barrier_semaphore()
    for dx in range(2):
        for de in range(4):
            for dz in range(4):
                if (dx, de, dz) != (0, 0, 0):
                    pl.semaphore_signal(bar, inc=1, device_id=ids((me_x + dx) % 2, (me_e + de) % 4, (me_z + dz) % 4), device_id_type=MESH_IDS)
    copy_a = pltpu.make_async_copy(a_hbm, a_v, sem_a)
    copy_a.start()
    for j in range(16):
        out_s[j] = x0_ref[:, j * 128:(j + 1) * 128]
        for a in range(2):
            for i in range(4):
                s0[a, i, :, j * 128:(j + 1) * 128] = out_s[j, pl.ds(2 * i + a, 12, stride=8), :]
    wall[me_z, 0] = w_ref[...]
    wall[me_z, 1] = u_ref[...]
    pl.semaphore_wait(bar, 31)

    def i_copy(a, i):
        return send(s0.at[a, i], r0.at[a, me_z], sem_is.at[a, i], sem_ir.at[a, me_z], ids(i // 2, me_e, 2 * me_x + i % 2))

    def i_arrive(a, m):
        return send(s0.at[a, 0], r0.at[a, m], sem_is.at[a, 0], sem_ir.at[a, m], ids(far, me_e, me_z))

    def x_copy(a, k):
        i = 2 * far + k
        return send(s0.at[a, i], relay.at[a, k], sem_is.at[a, i], sem_rr.at[a, k], ids(far, me_e, me_z))

    def r_copy(a, k):
        return send(relay.at[a, k], r0.at[a, me_z], sem_rs.at[a, k], sem_ir.at[a, me_z], ids(me_x, me_e, 2 * far + k))

    def b_copy(n):
        dev = ids(me_z // 2, me_e, 2 * me_x + low)
        return send(y_in, y_ref, sem_bs.at[0], sem_br.at[0], dev) if n == 0 else send(r_in, r_ref, sem_bs.at[1], sem_br.at[1], dev)

    def w_copy(dz, slot):
        tz = (me_z + dz) % 4
        return send(wall.at[me_z, core], wall.at[slot, core], sem_ws.at[tz], sem_wr.at[slot], ids(me_x, me_e, tz))

    def d_copy(q, c):
        return send(wall.at[q, c], wall.at[q, c], sem_ds.at[q], sem_dr.at[q], ids(me_x, mate, me_z))

    def start_init(a):
        @pl.when(inside)
        def _():
            for i in range(4):
                @pl.when(me_z != i)
                def _():
                    i_copy(a, i).start()
            r0[a, me_z] = s0[a, me_z]

        @pl.when(jnp.logical_not(inside))
        def _():
            for k in range(2):
                x_copy(a, k).start()
            for k in range(2):
                i_copy(a, 2 * me_x + k).start()

    def start_relay(a):
        @pl.when(inside)
        def _():
            for k in range(2):
                x_copy(a, k).wait_recv()
                r_copy(a, k).start()

    def end_init(a):
        @pl.when(inside)
        def _():
            for i in range(4):
                @pl.when(me_z != i)
                def _():
                    i_copy(a, i).wait_send()
            for k in range(2):
                r_copy(a, k).wait_send()

        @pl.when(jnp.logical_not(inside))
        def _():
            for k in range(2):
                x_copy(a, k).wait_send()
                i_copy(a, 2 * me_x + k).wait_send()

    start_init(0)
    for dz in (2, 1, 3):
        w_copy(dz, me_z).start()
    start_relay(0)
    start_init(1)

    @pl.when(inside)
    def _():
        y_ref[...] = y_in[...]
        r_ref[...] = r_in[...]

    @pl.when(jnp.logical_not(inside))
    def _():
        b_copy(0).start()
        b_copy(1).start()
    start_relay(1)

    copy_a.wait()
    row = lax.broadcasted_iota(jnp.int32, (256, 256), 0)
    col = lax.broadcasted_iota(jnp.int32, (256, 256), 1)
    eye = jnp.where(row == col, 1.0, 0.0).astype(BF16)

    def flip(i, carry):
        for j in range(8):
            tile = a_v[pl.ds(pl.multiple_of(i * 256, 256), 256), j * 256:(j + 1) * 256]
            at[j * 256:(j + 1) * 256, pl.ds(pl.multiple_of(i * 256, 256), 256)] = lax.dot_general(
                eye, tile, (((1,), (1,)), ((), ())), preferred_element_type=F32).astype(BF16)
        return carry

    lax.fori_loop(0, 8, flip, 0)

    for dz in (2, 1, 3):
        tz = (me_z + dz) % 4
        w_copy(dz, tz).wait()
        d_copy(tz, core).start()
    for dz in (2, 1, 3):
        tz = (me_z + dz) % 4
        d_copy(tz, core).wait_send()
        d_copy(tz, 1 - core).wait_recv()
    for l in range(layers):
        parts = [wall[q, 0, l].astype(F32) for q in range(4)]
        full = jnp.concatenate([jnp.concatenate(parts, axis=1), jnp.zeros((80, 768), F32)], axis=0)
        wt[l] = jnp.transpose(full).astype(BF16)
        ut[l] = jnp.concatenate([wall[q, 1, l].astype(F32) for q in range(4)], axis=1).astype(BF16)

    @pl.when(jnp.logical_not(inside))
    def _():
        b_copy(0).wait()
        b_copy(1).wait()

    def spot(b):
        tx = (me_x + (7 - b) // 4) % 2
        te = 2 * ((me_e // 2 + (7 - b) // 2) % 2) + (core + 7 - b) % 2
        return tx, te

    def pick(i):
        tx, te = spot(i // 2)
        tl = (low + i + 1) % 2
        return tx, te, tl, te * 4 + tx * 2 + tl

    def c_copy(a, tx, te, tl, slot):
        t = te * 4 + tx * 2 + tl
        return send(hw.at[a, :, pl.ds(pl.multiple_of(t * 128, 128), 128)], recv_c.at[slot, a],
                    sem_cs.at[a, t], sem_cr.at[a, slot], ids(tx, te, 2 * grp + tl))

    def f_copy(a, tx, te, tl, slot):
        t = te * 4 + tx * 2 + tl
        return send(send_f.at[a, t], recv_f.at[a, slot], sem_fs.at[a, t], sem_fr.at[a, slot], ids(tx, te, 2 * grp + tl))

    def o_copy(te, tz, slot):
        t = te * 4 + tz
        return send(out_s.at[t], out_r.at[:, pl.ds(pl.multiple_of(slot * 128, 128), 128)],
                    sem_os.at[t], sem_or.at[slot], ids(grp, te, tz))

    def others(fn):
        def body(i, carry):
            tx, te, tl, t = pick(i)

            @pl.when(t != me)
            def _():
                fn(tx, te, tl, t)
            return carry
        lax.fori_loop(0, 16, body, 0)

    def forecast(cyc, a):
        @pl.when(cyc == 0)
        def _():
            for q in range(4):
                @pl.when(jnp.logical_not(jnp.logical_and(inside, me_z == q)))
                def _():
                    i_arrive(a, q).wait_recv()
            for q in range(4):
                hw[a, q * 12:(q + 1) * 12, :] = r0[a, q]
            hb[0] = hw[a].astype(BF16)

        @pl.when(cyc > 0)
        def _():
            def drain(tx, te, tl, t):
                c_copy(a, tx, te, tl, t).wait_send()
                f_copy(a, tx, te, tl, t).wait()
            others(drain)

            def load(j, carry):
                sl = pl.ds(pl.multiple_of(j * 128, 128), 128)
                block = recv_f[a, j]
                hw[a, :, sl] = block
                hb[0, :, sl] = block.astype(BF16)
                return carry
            lax.fori_loop(0, 16, load, 0)

        pad = jnp.zeros((80, 256), BF16)

        def layer(l, carry):
            now = l % 2
            spots = [spot(b) for b in range(8)]
            slices = [pl.ds(pl.multiple_of((2 * te + tx) * 256, 256), 256) for tx, te in spots]

            def mixed(b):
                res = jnp.dot(hb[now], at[:, slices[b]], preferred_element_type=F32)
                return jnp.concatenate([res.astype(BF16), pad], axis=0)

            def sends(bs):
                @pl.when(l == layers - 1)
                def _():
                    for b in bs:
                        tx, te = spots[b]
                        for tl in range(2):
                            t = te * 4 + tx * 2 + tl

                            @pl.when(t != me)
                            def _():
                                c_copy(a, tx, te, tl, me).start()

                            @pl.when(t == me)
                            def _():
                                recv_c[me, a] = hw[a, :, pl.ds(pl.multiple_of(me * 128, 128), 128)]

            mix = mixed(0)
            for b in range(8):
                following = mixed(b + 1) if b < 7 else None
                parts = []
                for n in range(6):
                    hid = jnp.dot(wt[l, n * 128:(n + 1) * 128, :], mix, preferred_element_type=F32)
                    parts.append(gelu(hid).astype(BF16))
                upd = jnp.dot(ut[l], jnp.concatenate(parts, axis=0), preferred_element_type=F32)
                new = hw[a, :, slices[b]] + upd
                hw[a, :, slices[b]] = new
                hb[1 - now, :, slices[b]] = new.astype(BF16)
                mix = following
                if b == 3:
                    sends(range(4))
            sends(range(4, 8))
            return carry
        lax.fori_loop(0, layers, layer, 0)

    def mat(p_ref, rows):
        out = []
        for i in range(n_obs):
            acc = None
            for k in range(n_obs):
                term = p_ref[i, k:k + 1, :] * rows[k]
                acc = term if acc is None else acc + term
            out.append(acc)
        return out

    def vec(p_ref, x):
        acc = None
        for k in range(n_obs):
            term = x[k:k + 1, :] * p_ref[k]
            acc = term if acc is None else acc + term
        return acc

    sub = lax.broadcasted_iota(jnp.int32, (n_obs, 128), 0)
    units = [jnp.where(sub == i, 1.0, 0.0).astype(F32) for i in range(n_obs)]
    c0 = (members - 1) / rho_ref[0]

    def analyse(cyc):
        for a in range(2):
            others(lambda tx, te, tl, t: c_copy(a, tx, te, tl, t).wait_recv())

        def add(j, acc):
            return acc + (recv_c[j, 0] + recv_c[j, 1])
        mean = lax.fori_loop(0, 16, add, jnp.zeros((48, 128), F32)) * (1.0 / members)
        m_s[...] = mean

        def centre(j, carry):
            for a in range(2):
                recv_c[j, a] = recv_c[j, a] - mean
            return carry
        lax.fori_loop(0, 16, centre, 0)

        root = jnp.sqrt(r_ref[...])
        for p in range(n_obs):
            ip = idx_ref[p]
            v_s[:, :, p:p + 1, :] = recv_c[:, :, pl.ds(ip, 1), :] * root[p:p + 1, :]

        for base_p in range(0, n_obs, 6):
            def outer(j, accs):
                accs = list(accs)
                for a in range(2):
                    x = recv_c[j, a]
                    for p in range(6):
                        accs[p] = accs[p] + v_s[j, a, base_p + p:base_p + p + 1, :] * x
                return tuple(accs)
            sums = lax.fori_loop(0, 16, outer, tuple(jnp.zeros((48, 128), F32) for _ in range(6)))
            for p in range(6):
                f_s[base_p + p] = sums[p]

        gain = []
        for q in range(n_obs):
            iq = idx_ref[q]
            c_m[:, q:q + 1, :] = f_s[:, pl.ds(iq, 1), :] * root[q:q + 1, :]
            gain.append(root[q:q + 1, :] * (y_ref[cyc, q:q + 1, :] - m_s[pl.ds(iq, 1), :]))
        gain = jnp.concatenate(gain, axis=0)

        trace = None
        for p in range(n_obs):
            term = c_m[p, p:p + 1, :]
            trace = term if trace is None else trace + term
        trace = trace + members * c0
        inv = 1.0 / trace
        for p in range(n_obs):
            dn_m[p] = units[p] * inv
            dz_m[p] = jnp.zeros((n_obs, 128), F32)

        def step(i, carry):
            n, z = carry
            t = 1.5 - 0.5 * n
            c_rows = [c_m[k] for k in range(n_obs)]
            nc = mat(dn_m, c_rows)
            for p in range(n_obs):
                t_m[p] = t * units[p] - 0.5 * nc[p]
            tz = mat(t_m, [dz_m[k] for k in range(n_obs)])
            tt = mat(t_m, [t_m[k] for k in range(n_obs)])
            for p in range(n_obs):
                dz_m[p] = tz[p] - (0.5 * z) * dn_m[p]
                q_m[p] = tt[p] - (0.5 * n) * (t_m[p] + t * units[p])
            dn = mat(dn_m, [q_m[k] for k in range(n_obs)])
            for p in range(n_obs):
                dn_m[p] = dn[p]
            return n * t * t, t * z
        n, z = lax.fori_loop(0, NS_STEPS, step, (c0 * inv, jnp.ones((1, 128), F32)))

        rs = 1.0 / jnp.sqrt(trace)
        scale = float((members - 1) ** 0.5) * rs
        alpha = scale * z

        def apply_z(x):
            return z * x + vec(dz_m, vec(c_m, x))
        h = apply_z(apply_z(gain)) * inv

        base = m_s[...]
        for p in range(n_obs):
            base = base + h[p:p + 1, :] * f_s[p]
        m_s[...] = base
        for q in range(n_obs):
            acc = None
            for p in range(n_obs):
                term = (scale * dz_m[q, p:p + 1, :]) * f_s[p]
                acc = term if acc is None else acc + term
            ft_s[q] = acc

        def updated(t, a):
            acc = m_s[...] + alpha * recv_c[t, a]
            for q in range(n_obs):
                acc = acc + v_s[t, a, q:q + 1, :] * ft_s[q]
            return acc

        @pl.when(cyc < cycles - 1)
        def _():
            for a in range(2):
                def back(i, carry):
                    tx, te, tl, t = pick(i)
                    new = updated(t, a)

                    @pl.when(t != me)
                    def _():
                        send_f[a, t] = new
                        f_copy(a, tx, te, tl, me).start()

                    @pl.when(t == me)
                    def _():
                        recv_f[a, me] = new
                    return carry
                lax.fori_loop(0, 16, back, 0)

        @pl.when(cyc == cycles - 1)
        def _():
            def final(i, carry):
                te = (me_e + i) % 4
                for k in range(8):
                    new = updated(te * 4 + k // 2, k % 2)
                    for q in range(4):
                        out_s[te * 4 + q, pl.ds(k, 12, stride=8), :] = new[q * 12:(q + 1) * 12, :]
                for dz in (2, 1, 3, 0):
                    tz = (me_z + dz) % 4
                    own = jnp.logical_and(inside, jnp.logical_and(te == me_e, tz == me_z))

                    @pl.when(jnp.logical_not(own))
                    def _():
                        o_copy(te, tz, me).start()

                    @pl.when(own)
                    def _():
                        out_r[:, pl.ds(pl.multiple_of(me * 128, 128), 128)] = out_s[te * 4 + tz]
                return carry
            lax.fori_loop(0, 4, final, 0)

    def cycle(cyc, carry):
        def one(a, inner):
            forecast(cyc, a)
            return inner
        lax.fori_loop(0, 2, one, 0)
        analyse(cyc)
        return carry
    lax.fori_loop(0, cycles, cycle, 0)

    for a in range(2):
        others(lambda tx, te, tl, t: c_copy(a, tx, te, tl, t).wait_send())
        end_init(a)

    def finish(i, carry):
        own = jnp.logical_and(inside, i == me)

        @pl.when(jnp.logical_not(own))
        def _():
            o_copy(i // 4, i % 4, i).wait_recv()

        @pl.when(jnp.logical_not(jnp.logical_and(inside, i == me_e * 4 + me_z)))
        def _():
            o_copy(i // 4, i % 4, i).wait_send()
        return carry
    lax.fori_loop(0, 16, finish, 0)
    out_ref[...] = out_r[...]


def solution(mesh):
    def local_step(ens_local, mix_op, w_in, w_out, obs_val, obs_prec, obs_idx, inflation):
        cycles, layers = obs_val.shape[0], w_in.shape[0]
        n_obs = obs_idx.shape[0]
        x0 = jnp.transpose(ens_local, (2, 0, 1)).reshape(96, 2048)
        u_t = jnp.transpose(w_out, (0, 2, 1))
        yobs = jnp.transpose(obs_val, (0, 2, 1))
        rinv = jnp.transpose(obs_prec)
        vmem = pl.BlockSpec(memory_space=pltpu.VMEM)
        smem = pl.BlockSpec(memory_space=pltpu.SMEM)
        dma = pltpu.SemaphoreType.DMA
        out = pl.pallas_call(
            functools.partial(kernel, (cycles, layers, n_obs)),
            out_shape=jax.ShapeDtypeStruct((96, 2048), F32),
            in_specs=[smem, smem, vmem, pl.BlockSpec(memory_space=pl.ANY), vmem, vmem, vmem, vmem],
            out_specs=vmem,
            scratch_shapes=[
                pltpu.VMEM((2048, 2048), BF16),
                pltpu.VMEM((2048, 2048), BF16),
                pltpu.VMEM((4, 2, layers, 48, 192), BF16),
                pltpu.VMEM((layers, 768, 128), BF16),
                pltpu.VMEM((layers, 48, 768), BF16),
                pltpu.VMEM((2, 4, 12, 2048), F32),
                pltpu.VMEM((2, 4, 12, 2048), F32),
                pltpu.VMEM((2, 2, 12, 2048), F32),
                pltpu.VMEM((cycles, n_obs, 128), F32),
                pltpu.VMEM((n_obs, 128), F32),
                pltpu.VMEM((2, 48, 2048), F32),
                pltpu.VMEM((2, 48, 2048), BF16),
                pltpu.VMEM((16, 2, 48, 128), F32),
                pltpu.VMEM((2, 16, 48, 128), F32),
                pltpu.VMEM((2, 16, 48, 128), F32),
                pltpu.VMEM((16, 96, 128), F32),
                pltpu.VMEM((96, 2048), F32),
                pltpu.VMEM((16, 2, n_obs, 128), F32),
                pltpu.VMEM((n_obs, 48, 128), F32),
                pltpu.VMEM((n_obs, 48, 128), F32),
                pltpu.VMEM((48, 128), F32),
                pltpu.VMEM((n_obs, n_obs, 128), F32),
                pltpu.VMEM((n_obs, n_obs, 128), F32),
                pltpu.VMEM((n_obs, n_obs, 128), F32),
                pltpu.VMEM((n_obs, n_obs, 128), F32),
                pltpu.VMEM((n_obs, n_obs, 128), F32),
                dma(()),
                dma((4,)), dma((4,)), dma((4,)), dma((4,)), dma((2,)), dma((2,)),
                dma((2, 4)), dma((2, 4)), dma((2, 2)), dma((2, 2)),
                dma((2, 16)), dma((2, 16)),
                dma((2, 16)), dma((2, 16)),
                dma((16,)), dma((16,)),
            ],
            compiler_params=pltpu.CompilerParams(
                collective_id=0, has_side_effects=True, vmem_limit_bytes=60 * 1024 * 1024),
        )(obs_idx, inflation, x0, mix_op, w_in, u_t, yobs, rinv)
        return jnp.transpose(out.reshape(12, 8, 2048), (1, 2, 0))

    member_spec = P(("case", "ens"), None, "model")
    col_axes = ("case", "ens", "model")
    in_specs = (member_spec, P(None, None), P(None, None, "model"), P(None, "model", None), P(None, col_axes, None), P(col_axes, None), P(None), P(None))
    return jax.shard_map(local_step, mesh=mesh, in_specs=in_specs, out_specs=member_spec, check_vma=False)
```

```python
import functools

import jax
import jax.numpy as jnp
from jax import lax
from jax.experimental import pallas as pl
from jax.experimental.pallas import tpu as pltpu
from jax.sharding import PartitionSpec as P

NS_STEPS = 12
MESH_IDS = pl.DeviceIdType.MESH
F32 = jnp.float32
BF16 = jnp.bfloat16
C1 = 0.7978845608028654
C2 = 0.7978845608028654 * 0.044715


def gelu(x):
    th = jnp.tanh(x * (C1 + C2 * (x * x)))
    half = 0.5 * x
    return half + half * th


def kernel(dims, idx_ref, rho_ref, x0_ref, a_hbm, w_ref, u_ref, y_in, r_in, out_ref,
           a_v, at, wall, wt, ut, s0, r0, relay, y_ref, r_ref, hw, hb, mt, recv_c, recv_f, send_f, out_s, out_r,
           v_s, f_s, ft_s, m_s, c_m, dn_m, dz_m, t_m, q_m,
           sem_a, sem_zs, sem_wr, sem_hs, sem_vs, sem_ds, sem_dr, sem_bs, sem_br, sem_is, sem_ir, sem_rs, sem_rr,
           sem_cs, sem_cr, sem_fs, sem_fr, sem_os, sem_or):
    cycles, layers, n_obs = dims
    me_x = lax.axis_index("case")
    me_e = lax.axis_index("ens")
    me_z = lax.axis_index("model")
    grp = me_z // 2
    low = me_z % 2
    core = me_e % 2
    far = 1 - me_x
    mate = me_e + 1 - 2 * core
    me = me_e * 4 + me_x * 2 + low
    inside = grp == me_x
    members = 32

    def ids(tx, te, tz):
        return {"case": tx, "ens": te, "model": tz}

    def send(src, dst, ssem, rsem, dev):
        return pltpu.make_async_remote_copy(
            src_ref=src, dst_ref=dst, send_sem=ssem, recv_sem=rsem, device_id=dev, device_id_type=MESH_IDS)

    bar = pltpu.get_barrier_semaphore()
    for dx in range(2):
        for de in range(4):
            for dz in range(4):
                if (dx, de, dz) != (0, 0, 0):
                    pl.semaphore_signal(bar, inc=1, device_id=ids((me_x + dx) % 2, (me_e + de) % 4, (me_z + dz) % 4), device_id_type=MESH_IDS)
    copy_a = pltpu.make_async_copy(a_hbm, a_v, sem_a)
    copy_a.start()
    for j in range(16):
        out_s[j] = x0_ref[:, j * 128:(j + 1) * 128]
        for a in range(2):
            for i in range(4):
                s0[a, i, :, j * 128:(j + 1) * 128] = out_s[j, pl.ds(2 * i + a, 12, stride=8), :]
    wall[me_z, 0] = w_ref[...]
    wall[me_z, 1] = u_ref[...]
    pl.semaphore_wait(bar, 31)

    def i_copy(a, i):
        return send(s0.at[a, i], r0.at[a, me_z], sem_is.at[a, i], sem_ir.at[a, me_z], ids(i // 2, me_e, 2 * me_x + i % 2))

    def i_arrive(a, m):
        return send(s0.at[a, 0], r0.at[a, m], sem_is.at[a, 0], sem_ir.at[a, m], ids(far, me_e, me_z))

    def x_copy(a, k):
        i = 2 * far + k
        return send(s0.at[a, i], relay.at[a, k], sem_is.at[a, i], sem_rr.at[a, k], ids(far, me_e, me_z))

    def r_copy(a, k):
        return send(relay.at[a, k], r0.at[a, me_z], sem_rs.at[a, k], sem_ir.at[a, me_z], ids(me_x, me_e, 2 * far + k))

    def b_copy(n):
        dev = ids(me_z // 2, me_e, 2 * me_x + low)
        return send(y_in, y_ref, sem_bs.at[0], sem_br.at[0], dev) if n == 0 else send(r_in, r_ref, sem_bs.at[1], sem_br.at[1], dev)

    def home(l):
        return me_x == l % 2, me_e // 2 == (l // 2) % 2

    def z_copy(l, dz, slot):
        tz = (me_z + dz) % 4
        return send(wall.at[me_z, core, l], wall.at[slot, core, l], sem_zs.at[l, tz], sem_wr.at[l, slot], ids(me_x, me_e, tz))

    def h_copy(l, q):
        return send(wall.at[q, core, l], wall.at[q, core, l], sem_hs.at[l, q], sem_wr.at[l, q], ids(far, me_e, me_z))

    def v_copy(l, q):
        return send(wall.at[q, core, l], wall.at[q, core, l], sem_vs.at[l, q], sem_wr.at[l, q], ids(me_x, (me_e + 2) % 4, me_z))

    def d_copy(q, c):
        return send(wall.at[q, c], wall.at[q, c], sem_ds.at[q], sem_dr.at[q], ids(me_x, mate, me_z))

    shifts = (2, 1, 3)

    def w_stage(stage):
        for l in range(layers):
            on_x, on_y = home(l)
            away = jnp.logical_not(on_x)
            off = jnp.logical_not(on_y)
            first = jnp.logical_and(on_x, on_y)
            second = jnp.logical_and(away, on_y)
            if stage == 0:
                @pl.when(first)
                def _():
                    for dz in shifts:
                        z_copy(l, dz, me_z).start()
            if stage == 1:
                @pl.when(first)
                def _():
                    for dz in shifts:
                        q = (me_z + dz) % 4
                        z_copy(l, dz, q).wait()
                        h_copy(l, q).start()
                        v_copy(l, q).start()
            if stage == 2:
                @pl.when(second)
                def _():
                    for dz in shifts:
                        q = (me_z + dz) % 4
                        h_copy(l, q).wait_recv()
                        v_copy(l, q).start()
            if stage == 3:
                @pl.when(off)
                def _():
                    for dz in shifts:
                        v_copy(l, (me_z + dz) % 4).wait_recv()

                @pl.when(first)
                def _():
                    for dz in shifts:
                        h_copy(l, (me_z + dz) % 4).wait_send()

                @pl.when(on_y)
                def _():
                    for dz in shifts:
                        v_copy(l, (me_z + dz) % 4).wait_send()
        if stage == 3:
            for dz in shifts:
                d_copy((me_z + dz) % 4, core).start()
            for dz in shifts:
                q = (me_z + dz) % 4
                d_copy(q, core).wait_send()
                d_copy(q, 1 - core).wait_recv()

    def start_init(a):
        @pl.when(inside)
        def _():
            for i in range(4):
                @pl.when(me_z != i)
                def _():
                    i_copy(a, i).start()
            r0[a, me_z] = s0[a, me_z]

        @pl.when(jnp.logical_not(inside))
        def _():
            for k in range(2):
                x_copy(a, k).start()
            for k in range(2):
                i_copy(a, 2 * me_x + k).start()

    def start_relay(a):
        @pl.when(inside)
        def _():
            for k in range(2):
                x_copy(a, k).wait_recv()
                r_copy(a, k).start()

    def end_init(a):
        @pl.when(inside)
        def _():
            for i in range(4):
                @pl.when(me_z != i)
                def _():
                    i_copy(a, i).wait_send()
            for k in range(2):
                r_copy(a, k).wait_send()

        @pl.when(jnp.logical_not(inside))
        def _():
            for k in range(2):
                x_copy(a, k).wait_send()
                i_copy(a, 2 * me_x + k).wait_send()

    w_stage(0)
    start_init(0)

    @pl.when(inside)
    def _():
        y_ref[...] = y_in[...]
        r_ref[...] = r_in[...]

    @pl.when(jnp.logical_not(inside))
    def _():
        b_copy(0).start()
        b_copy(1).start()
    mt[48:128, :] = jnp.zeros((80, 2048), BF16)

    copy_a.wait()
    row = lax.broadcasted_iota(jnp.int32, (256, 256), 0)
    col = lax.broadcasted_iota(jnp.int32, (256, 256), 1)
    eye = jnp.where(row == col, 1.0, 0.0).astype(BF16)

    def flip(i, carry):
        for j in range(8):
            tile = a_v[pl.ds(pl.multiple_of(i * 256, 256), 256), j * 256:(j + 1) * 256]
            at[j * 256:(j + 1) * 256, pl.ds(pl.multiple_of(i * 256, 256), 256)] = lax.dot_general(
                eye, tile, (((1,), (1,)), ((), ())), preferred_element_type=F32).astype(BF16)
        return carry

    w_stage(1)
    start_relay(0)
    w_stage(2)
    start_init(1)
    lax.fori_loop(0, 8, flip, 0)
    w_stage(3)
    start_relay(1)

    for l in range(layers):
        parts = [wall[q, 0, l].astype(F32) for q in range(4)]
        full = jnp.concatenate([jnp.concatenate(parts, axis=1), jnp.zeros((80, 768), F32)], axis=0)
        wt[l] = jnp.transpose(full).astype(BF16)
        ut[l] = jnp.concatenate([wall[q, 1, l].astype(F32) for q in range(4)], axis=1).astype(BF16)

    @pl.when(jnp.logical_not(inside))
    def _():
        b_copy(0).wait()
        b_copy(1).wait()

    def spot(b):
        tx = (me_x + (7 - b) // 4) % 2
        te = 2 * ((me_e // 2 + (7 - b) // 2) % 2) + (core + 7 - b) % 2
        return tx, te

    def pick(i):
        tx, te = spot(i // 2)
        tl = (low + i + 1) % 2
        return tx, te, tl, te * 4 + tx * 2 + tl

    def c_copy(a, tx, te, tl, slot):
        t = te * 4 + tx * 2 + tl
        return send(hw.at[a, :, pl.ds(pl.multiple_of(t * 128, 128), 128)], recv_c.at[slot, a],
                    sem_cs.at[a, t], sem_cr.at[a, slot], ids(tx, te, 2 * grp + tl))

    def f_copy(a, tx, te, tl, slot):
        t = te * 4 + tx * 2 + tl
        return send(send_f.at[a, t], recv_f.at[a, slot], sem_fs.at[a, t], sem_fr.at[a, slot], ids(tx, te, 2 * grp + tl))

    def o_copy(te, tz, slot):
        t = te * 4 + tz
        return send(out_s.at[t], out_r.at[:, pl.ds(pl.multiple_of(slot * 128, 128), 128)],
                    sem_os.at[t], sem_or.at[slot], ids(grp, te, tz))

    def others(fn):
        def body(i, carry):
            tx, te, tl, t = pick(i)

            @pl.when(t != me)
            def _():
                fn(tx, te, tl, t)
            return carry
        lax.fori_loop(0, 16, body, 0)

    def forecast(cyc, a):
        @pl.when(cyc == 0)
        def _():
            for q in range(4):
                @pl.when(jnp.logical_not(jnp.logical_and(inside, me_z == q)))
                def _():
                    i_arrive(a, q).wait_recv()
            for q in range(4):
                hw[a, q * 12:(q + 1) * 12, :] = r0[a, q]
            hb[...] = hw[a].astype(BF16)

        @pl.when(cyc > 0)
        def _():
            def drain(tx, te, tl, t):
                c_copy(a, tx, te, tl, t).wait_send()
                f_copy(a, tx, te, tl, t).wait()
            others(drain)

            def load(j, carry):
                sl = pl.ds(pl.multiple_of(j * 128, 128), 128)
                block = recv_f[a, j]
                hw[a, :, sl] = block
                hb[:, sl] = block.astype(BF16)
                return carry
            lax.fori_loop(0, 16, load, 0)

        def mix_all():
            for n in range(2):
                sl = slice(n * 1024, (n + 1) * 1024)
                mt[0:48, sl] = jnp.dot(hb[...], at[:, sl], preferred_element_type=F32).astype(BF16)

        def tile(l, sl):
            mix = mt[:, sl]
            parts = []
            for n in range(6):
                hid = jnp.dot(wt[l, n * 128:(n + 1) * 128, :], mix, preferred_element_type=F32)
                parts.append(gelu(hid).astype(BF16))
            upd = jnp.dot(ut[l], jnp.concatenate(parts, axis=0), preferred_element_type=F32)
            new = hw[a, :, sl] + upd
            hw[a, :, sl] = new
            return new

        def layer(l, carry):
            mix_all()
            for b in range(8):
                sl = slice(b * 256, (b + 1) * 256)
                hb[:, sl] = tile(l, sl).astype(BF16)
            return carry
        lax.fori_loop(0, layers - 1, layer, 0)

        def sends(b):
            tx, te = spot(b)
            for tl in ((1 - low, low) if b < 7 else (1 - low,)):
                c_copy(a, tx, te, tl, me).start()

        mix_all()
        for b in range(8):
            tx, te = spot(b)
            tile(layers - 1, pl.ds(pl.multiple_of((2 * te + tx) * 256, 256), 256))
            if b % 4 == 3:
                for n in range(b - 3, b + 1):
                    sends(n)
        recv_c[me, a] = hw[a, :, pl.ds(pl.multiple_of(me * 128, 128), 128)]

    def mat(p_ref, rows):
        out = []
        for i in range(n_obs):
            acc = None
            for k in range(n_obs):
                term = p_ref[i, k:k + 1, :] * rows[k]
                acc = term if acc is None else acc + term
            out.append(acc)
        return out

    def vec(p_ref, x):
        acc = None
        for k in range(n_obs):
            term = x[k:k + 1, :] * p_ref[k]
            acc = term if acc is None else acc + term
        return acc

    sub = lax.broadcasted_iota(jnp.int32, (n_obs, 128), 0)
    units = [jnp.where(sub == i, 1.0, 0.0).astype(F32) for i in range(n_obs)]
    c0 = (members - 1) / rho_ref[0]

    def analyse(cyc):
        for a in range(2):
            others(lambda tx, te, tl, t: c_copy(a, tx, te, tl, t).wait_recv())

        def add(j, acc):
            return acc + (recv_c[j, 0] + recv_c[j, 1])
        mean = lax.fori_loop(0, 16, add, jnp.zeros((48, 128), F32)) * (1.0 / members)
        m_s[...] = mean

        def centre(j, carry):
            for a in range(2):
                recv_c[j, a] = recv_c[j, a] - mean
            return carry
        lax.fori_loop(0, 16, centre, 0)

        root = jnp.sqrt(r_ref[...])
        for p in range(n_obs):
            ip = idx_ref[p]
            v_s[:, :, p:p + 1, :] = recv_c[:, :, pl.ds(ip, 1), :] * root[p:p + 1, :]

        for base_p in range(0, n_obs, 6):
            def outer(j, accs):
                accs = list(accs)
                for a in range(2):
                    x = recv_c[j, a]
                    for p in range(6):
                        accs[p] = accs[p] + v_s[j, a, base_p + p:base_p + p + 1, :] * x
                return tuple(accs)
            sums = lax.fori_loop(0, 16, outer, tuple(jnp.zeros((48, 128), F32) for _ in range(6)))
            for p in range(6):
                f_s[base_p + p] = sums[p]

        gain = []
        for q in range(n_obs):
            iq = idx_ref[q]
            c_m[:, q:q + 1, :] = f_s[:, pl.ds(iq, 1), :] * root[q:q + 1, :]
            gain.append(root[q:q + 1, :] * (y_ref[cyc, q:q + 1, :] - m_s[pl.ds(iq, 1), :]))
        gain = jnp.concatenate(gain, axis=0)

        trace = None
        for p in range(n_obs):
            term = c_m[p, p:p + 1, :]
            trace = term if trace is None else trace + term
        trace = trace + members * c0
        inv = 1.0 / trace
        n0 = c0 * inv
        t0 = 1.5 - 0.5 * n0
        for p in range(n_obs):
            dz_m[p] = units[p] * (-0.5 * inv)
            t_m[p] = t0 * units[p] - (0.5 * inv) * c_m[p]
        tt = mat(t_m, [t_m[k] for k in range(n_obs)])
        for p in range(n_obs):
            dn_m[p] = inv * (tt[p] - (0.5 * n0) * (t_m[p] + t0 * units[p]))

        def half_step(n, z):
            t = 1.5 - 0.5 * n
            nc = mat(dn_m, [c_m[k] for k in range(n_obs)])
            for p in range(n_obs):
                t_m[p] = t * units[p] - 0.5 * nc[p]
            tz = mat(t_m, [dz_m[k] for k in range(n_obs)])
            for p in range(n_obs):
                dz_m[p] = tz[p] - (0.5 * z) * dn_m[p]
            return t

        def step(i, carry):
            n, z = carry
            t = half_step(n, z)
            tt = mat(t_m, [t_m[k] for k in range(n_obs)])
            for p in range(n_obs):
                q_m[p] = tt[p] - (0.5 * n) * (t_m[p] + t * units[p])
            dn = mat(dn_m, [q_m[k] for k in range(n_obs)])
            for p in range(n_obs):
                dn_m[p] = dn[p]
            return n * t * t, t * z
        n, z = lax.fori_loop(1, NS_STEPS - 1, step, (n0 * t0 * t0, t0))
        z = half_step(n, z) * z

        rs = 1.0 / jnp.sqrt(trace)
        scale = float((members - 1) ** 0.5) * rs
        alpha = scale * z

        def apply_z(x):
            return z * x + vec(dz_m, vec(c_m, x))
        h = apply_z(apply_z(gain)) * inv

        base = m_s[...]
        for p in range(n_obs):
            base = base + h[p:p + 1, :] * f_s[p]
        m_s[...] = base
        for q in range(n_obs):
            acc = None
            for p in range(n_obs):
                term = (scale * dz_m[q, p:p + 1, :]) * f_s[p]
                acc = term if acc is None else acc + term
            ft_s[q] = acc

        def updated(t, a):
            acc = m_s[...] + alpha * recv_c[t, a]
            for q in range(n_obs):
                acc = acc + v_s[t, a, q:q + 1, :] * ft_s[q]
            return acc

        @pl.when(cyc < cycles - 1)
        def _():
            for a in range(2):
                def back(i, carry):
                    tx, te, tl, t = pick(i)
                    new = updated(t, a)

                    @pl.when(t != me)
                    def _():
                        send_f[a, t] = new
                        f_copy(a, tx, te, tl, me).start()

                    @pl.when(t == me)
                    def _():
                        recv_f[a, me] = new
                    return carry
                lax.fori_loop(0, 16, back, 0)

        @pl.when(cyc == cycles - 1)
        def _():
            def final(i, carry):
                te = (me_e + i) % 4
                for k in range(8):
                    new = updated(te * 4 + k // 2, k % 2)
                    for q in range(4):
                        out_s[te * 4 + q, pl.ds(k, 12, stride=8), :] = new[q * 12:(q + 1) * 12, :]
                for dz in (2, 1, 3, 0):
                    tz = (me_z + dz) % 4
                    own = jnp.logical_and(inside, jnp.logical_and(te == me_e, tz == me_z))

                    @pl.when(jnp.logical_not(own))
                    def _():
                        o_copy(te, tz, me).start()

                    @pl.when(own)
                    def _():
                        out_r[:, pl.ds(pl.multiple_of(me * 128, 128), 128)] = out_s[te * 4 + tz]
                return carry
            lax.fori_loop(0, 4, final, 0)

    def cycle(cyc, carry):
        def one(a, inner):
            forecast(cyc, a)
            return inner
        lax.fori_loop(0, 2, one, 0)
        analyse(cyc)
        return carry
    lax.fori_loop(0, cycles, cycle, 0)

    for a in range(2):
        others(lambda tx, te, tl, t: c_copy(a, tx, te, tl, t).wait_send())
        end_init(a)

    def finish(i, carry):
        own = jnp.logical_and(inside, i == me)

        @pl.when(jnp.logical_not(own))
        def _():
            o_copy(i // 4, i % 4, i).wait_recv()

        @pl.when(jnp.logical_not(jnp.logical_and(inside, i == me_e * 4 + me_z)))
        def _():
            o_copy(i // 4, i % 4, i).wait_send()
        return carry
    lax.fori_loop(0, 16, finish, 0)
    out_ref[...] = out_r[...]


def solution(mesh):
    def local_step(ens_local, mix_op, w_in, w_out, obs_val, obs_prec, obs_idx, inflation):
        cycles, layers = obs_val.shape[0], w_in.shape[0]
        n_obs = obs_idx.shape[0]
        x0 = jnp.transpose(ens_local, (2, 0, 1)).reshape(96, 2048)
        u_t = jnp.transpose(w_out, (0, 2, 1))
        yobs = jnp.transpose(obs_val, (0, 2, 1))
        rinv = jnp.transpose(obs_prec)
        vmem = pl.BlockSpec(memory_space=pltpu.VMEM)
        smem = pl.BlockSpec(memory_space=pltpu.SMEM)
        dma = pltpu.SemaphoreType.DMA
        out = pl.pallas_call(
            functools.partial(kernel, (cycles, layers, n_obs)),
            out_shape=jax.ShapeDtypeStruct((96, 2048), F32),
            in_specs=[smem, smem, vmem, pl.BlockSpec(memory_space=pl.ANY), vmem, vmem, vmem, vmem],
            out_specs=vmem,
            scratch_shapes=[
                pltpu.VMEM((2048, 2048), BF16),
                pltpu.VMEM((2048, 2048), BF16),
                pltpu.VMEM((4, 2, layers, 48, 192), BF16),
                pltpu.VMEM((layers, 768, 128), BF16),
                pltpu.VMEM((layers, 48, 768), BF16),
                pltpu.VMEM((2, 4, 12, 2048), F32),
                pltpu.VMEM((2, 4, 12, 2048), F32),
                pltpu.VMEM((2, 2, 12, 2048), F32),
                pltpu.VMEM((cycles, n_obs, 128), F32),
                pltpu.VMEM((n_obs, 128), F32),
                pltpu.VMEM((2, 48, 2048), F32),
                pltpu.VMEM((48, 2048), BF16),
                pltpu.VMEM((128, 2048), BF16),
                pltpu.VMEM((16, 2, 48, 128), F32),
                pltpu.VMEM((2, 16, 48, 128), F32),
                pltpu.VMEM((2, 16, 48, 128), F32),
                pltpu.VMEM((16, 96, 128), F32),
                pltpu.VMEM((96, 2048), F32),
                pltpu.VMEM((16, 2, n_obs, 128), F32),
                pltpu.VMEM((n_obs, 48, 128), F32),
                pltpu.VMEM((n_obs, 48, 128), F32),
                pltpu.VMEM((48, 128), F32),
                pltpu.VMEM((n_obs, n_obs, 128), F32),
                pltpu.VMEM((n_obs, n_obs, 128), F32),
                pltpu.VMEM((n_obs, n_obs, 128), F32),
                pltpu.VMEM((n_obs, n_obs, 128), F32),
                pltpu.VMEM((n_obs, n_obs, 128), F32),
                dma(()),
                dma((layers, 4)), dma((layers, 4)), dma((layers, 4)), dma((layers, 4)),
                dma((4,)), dma((4,)), dma((2,)), dma((2,)),
                dma((2, 4)), dma((2, 4)), dma((2, 2)), dma((2, 2)),
                dma((2, 16)), dma((2, 16)),
                dma((2, 16)), dma((2, 16)),
                dma((16,)), dma((16,)),
            ],
            compiler_params=pltpu.CompilerParams(
                collective_id=0, has_side_effects=True, vmem_limit_bytes=60 * 1024 * 1024),
        )(obs_idx, inflation, x0, mix_op, w_in, u_t, yobs, rinv)
        return jnp.transpose(out.reshape(12, 8, 2048), (1, 2, 0))

    member_spec = P(("case", "ens"), None, "model")
    col_axes = ("case", "ens", "model")
    in_specs = (member_spec, P(None, None), P(None, None, "model"), P(None, "model", None), P(None, col_axes, None), P(col_axes, None), P(None), P(None))
    return jax.shard_map(local_step, mesh=mesh, in_specs=in_specs, out_specs=member_spec, check_vma=False)
```

```python
import functools

import jax
import jax.numpy as jnp
from jax import lax
from jax.experimental import pallas as pl
from jax.experimental.pallas import tpu as pltpu
from jax.sharding import PartitionSpec as P

NS_STEPS = 12
MESH_IDS = pl.DeviceIdType.MESH
F32 = jnp.float32
BF16 = jnp.bfloat16
C1 = 0.7978845608028654
C2 = 0.7978845608028654 * 0.044715


def gelu(x):
    th = jnp.tanh(x * (C1 + C2 * (x * x)))
    half = 0.5 * x
    return half + half * th


def kernel(dims, idx_ref, rho_ref, x0_ref, a_hbm, w_ref, u_ref, y_in, r_in, out_ref,
           a_v, at, wall, wt, ut, s0, r0, relay, y_ref, r_ref, hw, hb, mt, recv_c, recv_f, send_f, out_s, out_r,
           x_s, v_s, f_s, ft_s, m_s, d_s, b_s, c_m, dn_m, dz_m, t_m, q_m,
           sem_a, sem_zs, sem_wr, sem_hs, sem_vs, sem_ds, sem_dr, sem_bs, sem_br, sem_is, sem_ir, sem_rs, sem_rr,
           sem_cs, sem_cr, sem_fs, sem_fr, sem_os, sem_or):
    cycles, layers, n_obs = dims
    me_x = lax.axis_index("case")
    me_e = lax.axis_index("ens")
    me_z = lax.axis_index("model")
    grp = me_z // 2
    low = me_z % 2
    core = me_e % 2
    far = 1 - me_x
    mate = me_e + 1 - 2 * core
    me = me_e * 4 + me_x * 2 + low
    inside = grp == me_x
    members = 32

    def ids(tx, te, tz):
        return {"case": tx, "ens": te, "model": tz}

    def send(src, dst, ssem, rsem, dev):
        return pltpu.make_async_remote_copy(
            src_ref=src, dst_ref=dst, send_sem=ssem, recv_sem=rsem, device_id=dev, device_id_type=MESH_IDS)

    bar = pltpu.get_barrier_semaphore()
    for dx in range(2):
        for de in range(4):
            for dz in range(4):
                if (dx, de, dz) != (0, 0, 0):
                    pl.semaphore_signal(bar, inc=1, device_id=ids((me_x + dx) % 2, (me_e + de) % 4, (me_z + dz) % 4), device_id_type=MESH_IDS)
    copy_a = pltpu.make_async_copy(a_hbm, a_v, sem_a)
    copy_a.start()
    for j in range(16):
        out_s[j] = x0_ref[:, j * 128:(j + 1) * 128]
        for a in range(2):
            for i in range(4):
                s0[a, i, :, j * 128:(j + 1) * 128] = out_s[j, pl.ds(2 * i + a, 12, stride=8), :]
    wall[me_z, 0] = w_ref[...]
    wall[me_z, 1] = u_ref[...]
    pl.semaphore_wait(bar, 31)

    def i_copy(a, i):
        return send(s0.at[a, i], r0.at[a, me_z], sem_is.at[a, i], sem_ir.at[a, me_z], ids(i // 2, me_e, 2 * me_x + i % 2))

    def i_arrive(a, m):
        return send(s0.at[a, 0], r0.at[a, m], sem_is.at[a, 0], sem_ir.at[a, m], ids(far, me_e, me_z))

    def x_copy(a, k):
        i = 2 * far + k
        return send(s0.at[a, i], relay.at[a, k], sem_is.at[a, i], sem_rr.at[a, k], ids(far, me_e, me_z))

    def r_copy(a, k):
        return send(relay.at[a, k], r0.at[a, me_z], sem_rs.at[a, k], sem_ir.at[a, me_z], ids(me_x, me_e, 2 * far + k))

    def b_copy(n):
        dev = ids(me_z // 2, me_e, 2 * me_x + low)
        return send(y_in, y_ref, sem_bs.at[0], sem_br.at[0], dev) if n == 0 else send(r_in, r_ref, sem_bs.at[1], sem_br.at[1], dev)

    def home(l):
        return me_x == l % 2, me_e // 2 == (l // 2) % 2

    def z_copy(l, dz, slot):
        tz = (me_z + dz) % 4
        return send(wall.at[me_z, core, l], wall.at[slot, core, l], sem_zs.at[l, tz], sem_wr.at[l, slot], ids(me_x, me_e, tz))

    def h_copy(l, q):
        return send(wall.at[q, core, l], wall.at[q, core, l], sem_hs.at[l, q], sem_wr.at[l, q], ids(far, me_e, me_z))

    def v_copy(l, q):
        return send(wall.at[q, core, l], wall.at[q, core, l], sem_vs.at[l, q], sem_wr.at[l, q], ids(me_x, (me_e + 2) % 4, me_z))

    def d_copy(q, c):
        return send(wall.at[q, c], wall.at[q, c], sem_ds.at[q], sem_dr.at[q], ids(me_x, mate, me_z))

    shifts = (2, 1, 3)

    def w_stage(stage):
        for l in range(layers):
            on_x, on_y = home(l)
            away = jnp.logical_not(on_x)
            off = jnp.logical_not(on_y)
            first = jnp.logical_and(on_x, on_y)
            second = jnp.logical_and(away, on_y)
            if stage == 0:
                @pl.when(first)
                def _():
                    for dz in shifts:
                        z_copy(l, dz, me_z).start()
            if stage == 1:
                @pl.when(first)
                def _():
                    for dz in shifts:
                        q = (me_z + dz) % 4
                        z_copy(l, dz, q).wait()
                        h_copy(l, q).start()
                        v_copy(l, q).start()
            if stage == 2:
                @pl.when(second)
                def _():
                    for dz in shifts:
                        q = (me_z + dz) % 4
                        h_copy(l, q).wait_recv()
                        v_copy(l, q).start()
            if stage == 3:
                @pl.when(off)
                def _():
                    for dz in shifts:
                        v_copy(l, (me_z + dz) % 4).wait_recv()

                @pl.when(first)
                def _():
                    for dz in shifts:
                        h_copy(l, (me_z + dz) % 4).wait_send()

                @pl.when(on_y)
                def _():
                    for dz in shifts:
                        v_copy(l, (me_z + dz) % 4).wait_send()
        if stage == 3:
            for dz in shifts:
                d_copy((me_z + dz) % 4, core).start()
            for dz in shifts:
                q = (me_z + dz) % 4
                d_copy(q, core).wait_send()
                d_copy(q, 1 - core).wait_recv()

    def start_init(a):
        @pl.when(inside)
        def _():
            for i in range(4):
                @pl.when(me_z != i)
                def _():
                    i_copy(a, i).start()
            r0[a, me_z] = s0[a, me_z]

        @pl.when(jnp.logical_not(inside))
        def _():
            for k in range(2):
                x_copy(a, k).start()
            for k in range(2):
                i_copy(a, 2 * me_x + k).start()

    def start_relay(a):
        @pl.when(inside)
        def _():
            for k in range(2):
                x_copy(a, k).wait_recv()
                r_copy(a, k).start()

    def end_init(a):
        @pl.when(inside)
        def _():
            for i in range(4):
                @pl.when(me_z != i)
                def _():
                    i_copy(a, i).wait_send()
            for k in range(2):
                r_copy(a, k).wait_send()

        @pl.when(jnp.logical_not(inside))
        def _():
            for k in range(2):
                x_copy(a, k).wait_send()
                i_copy(a, 2 * me_x + k).wait_send()

    w_stage(0)
    start_init(0)

    @pl.when(inside)
    def _():
        y_ref[...] = y_in[...]
        r_ref[...] = r_in[...]

    @pl.when(jnp.logical_not(inside))
    def _():
        b_copy(0).start()
        b_copy(1).start()
    mt[48:128, :] = jnp.zeros((80, 2048), BF16)

    copy_a.wait()
    row = lax.broadcasted_iota(jnp.int32, (256, 256), 0)
    col = lax.broadcasted_iota(jnp.int32, (256, 256), 1)
    eye = jnp.where(row == col, 1.0, 0.0).astype(BF16)

    def flip(i, carry):
        for j in range(8):
            tile = a_v[pl.ds(pl.multiple_of(i * 256, 256), 256), j * 256:(j + 1) * 256]
            at[j * 256:(j + 1) * 256, pl.ds(pl.multiple_of(i * 256, 256), 256)] = lax.dot_general(
                eye, tile, (((1,), (1,)), ((), ())), preferred_element_type=F32).astype(BF16)
        return carry

    w_stage(1)
    start_relay(0)
    w_stage(2)
    start_init(1)
    lax.fori_loop(0, 8, flip, 0)
    w_stage(3)
    start_relay(1)

    for l in range(layers):
        parts = [wall[q, 0, l].astype(F32) for q in range(4)]
        full = jnp.concatenate([jnp.concatenate(parts, axis=1), jnp.zeros((80, 768), F32)], axis=0)
        wt[l] = jnp.transpose(full).astype(BF16)
        ut[l] = jnp.concatenate([wall[q, 1, l].astype(F32) for q in range(4)], axis=1).astype(BF16)

    @pl.when(jnp.logical_not(inside))
    def _():
        b_copy(0).wait()
        b_copy(1).wait()

    def spot(b):
        tx = (me_x + (7 - b) // 4) % 2
        te = 2 * ((me_e // 2 + (7 - b) // 2) % 2) + (core + 7 - b) % 2
        return tx, te

    def pick(i):
        tx, te = spot(i // 2)
        tl = (low + i + 1) % 2
        return tx, te, tl, te * 4 + tx * 2 + tl

    def c_copy(a, tx, te, tl, slot):
        t = te * 4 + tx * 2 + tl
        return send(hw.at[a, :, pl.ds(pl.multiple_of(t * 128, 128), 128)], recv_c.at[slot, a],
                    sem_cs.at[a], sem_cr.at[a], ids(tx, te, 2 * grp + tl))

    def f_copy(a, tx, te, tl, slot):
        t = te * 4 + tx * 2 + tl
        return send(send_f.at[a, t], recv_f.at[a, slot], sem_fs.at[a], sem_fr.at[a], ids(tx, te, 2 * grp + tl))

    def o_copy(te, tz, slot):
        t = te * 4 + tz
        return send(out_s.at[t], out_r.at[:, pl.ds(pl.multiple_of(slot * 128, 128), 128)],
                    sem_os, sem_or, ids(grp, te, tz))

    def c_all(a):
        return send(recv_c.at[0:15, a], recv_c.at[0:15, a], sem_cs.at[a], sem_cr.at[a], ids(far, me_e, me_z))

    def f_all(a):
        return send(send_f.at[a, 0:15], recv_f.at[a, 0:15], sem_fs.at[a], sem_fr.at[a], ids(far, me_e, me_z))

    def o_all(n):
        return send(out_s.at[0:n], out_s.at[0:n], sem_os, sem_or, ids(far, me_e, me_z))

    def forecast(cyc, a):
        @pl.when(cyc == 0)
        def _():
            for q in range(4):
                @pl.when(jnp.logical_not(jnp.logical_and(inside, me_z == q)))
                def _():
                    i_arrive(a, q).wait_recv()
            for q in range(4):
                hw[a, q * 12:(q + 1) * 12, :] = r0[a, q]
            hb[...] = hw[a].astype(BF16)

        @pl.when(cyc > 0)
        def _():
            c_all(a).wait_send()
            f_all(a).wait()
            for j in range(16):
                sl = slice(j * 128, (j + 1) * 128)
                block = recv_f[a, j]
                hw[a, :, sl] = block
                hb[:, sl] = block.astype(BF16)

        def mix_all():
            for n in range(2):
                sl = slice(n * 1024, (n + 1) * 1024)
                mt[0:48, sl] = jnp.dot(hb[...], at[:, sl], preferred_element_type=F32).astype(BF16)

        def tile(l, sl):
            mix = mt[:, sl]
            parts = []
            for n in range(6):
                hid = jnp.dot(wt[l, n * 128:(n + 1) * 128, :], mix, preferred_element_type=F32)
                parts.append(gelu(hid).astype(BF16))
            upd = jnp.dot(ut[l], jnp.concatenate(parts, axis=0), preferred_element_type=F32)
            new = hw[a, :, sl] + upd
            hw[a, :, sl] = new
            return new

        def layer(l, carry):
            mix_all()
            for b in range(8):
                sl = slice(b * 256, (b + 1) * 256)
                hb[:, sl] = tile(l, sl).astype(BF16)
            return carry
        lax.fori_loop(0, layers - 1, layer, 0)

        def sends(b):
            tx, te = spot(b)
            for tl in ((1 - low, low) if b < 7 else (1 - low,)):
                c_copy(a, tx, te, tl, me).start()

        mix_all()
        for b in range(8):
            tx, te = spot(b)
            tile(layers - 1, pl.ds(pl.multiple_of((2 * te + tx) * 256, 256), 256))
            if b % 4 == 3:
                for n in range(b - 3, b + 1):
                    sends(n)
        recv_c[me, a] = hw[a, :, pl.ds(pl.multiple_of(me * 128, 128), 128)]

    def mat(p_ref, rows):
        out = []
        for i in range(n_obs):
            acc = None
            for k in range(n_obs):
                term = p_ref[i, k:k + 1, :] * rows[k]
                acc = term if acc is None else acc + term
            out.append(acc)
        return out

    def vec(p_ref, x):
        acc = None
        for k in range(n_obs):
            term = x[k:k + 1, :] * p_ref[k]
            acc = term if acc is None else acc + term
        return acc

    sub = lax.broadcasted_iota(jnp.int32, (n_obs, 128), 0)
    units = [jnp.where(sub == i, 1.0, 0.0).astype(F32) for i in range(n_obs)]
    c0 = (members - 1) / rho_ref[0]

    def analyse(cyc):
        root = jnp.sqrt(r_ref[...])
        means = []
        for a in range(2):
            c_all(a).wait_recv()

            def add(j, acc):
                return acc + ((recv_c[4 * j, a] + recv_c[4 * j + 1, a]) + (recv_c[4 * j + 2, a] + recv_c[4 * j + 3, a]))
            part = lax.fori_loop(0, 4, add, jnp.zeros((48, 128), F32)) * (2.0 / members)
            means.append(part)

            def centre(j, carry):
                for n in range(4):
                    block = recv_c[4 * j + n, a] - part
                    recv_c[4 * j + n, a] = block
                    x_s[4 * j + n] = block
                return carry
            lax.fori_loop(0, 4, centre, 0)

            for p in range(n_obs):
                ip = idx_ref[p]
                v_s[:, a, p:p + 1, :] = x_s[:, pl.ds(ip, 1), :] * root[p:p + 1, :]

            for base_p in range(0, n_obs, 6):
                def outer(j, accs):
                    accs = list(accs)
                    for n in range(2):
                        x = recv_c[2 * j + n, a]
                        for p in range(6):
                            accs[p] = accs[p] + v_s[2 * j + n, a, base_p + p:base_p + p + 1, :] * x
                    return tuple(accs)
                start = tuple(jnp.zeros((48, 128), F32) if a == 0 else f_s[base_p + p] for p in range(6))
                sums = lax.fori_loop(0, 8, outer, start)
                for p in range(6):
                    f_s[base_p + p] = sums[p]

        mean = 0.5 * (means[0] + means[1])
        delta = 0.5 * (means[0] - means[1])
        m_s[...] = mean
        d_s[...] = delta
        shift = [root[p:p + 1, :] * d_s[pl.ds(idx_ref[p], 1), :] for p in range(n_obs)]
        for p in range(n_obs):
            f_s[p] = f_s[p] + (float(members) * shift[p]) * delta

        gain = []
        for q in range(n_obs):
            iq = idx_ref[q]
            c_m[:, q:q + 1, :] = f_s[:, pl.ds(iq, 1), :] * root[q:q + 1, :]
            gain.append(root[q:q + 1, :] * (y_ref[cyc, q:q + 1, :] - m_s[pl.ds(iq, 1), :]))
        gain = jnp.concatenate(gain, axis=0)

        trace = None
        for p in range(n_obs):
            term = c_m[p, p:p + 1, :]
            trace = term if trace is None else trace + term
        trace = trace + members * c0
        inv = 1.0 / trace
        n0 = c0 * inv
        t0 = 1.5 - 0.5 * n0
        for p in range(n_obs):
            dz_m[p] = units[p] * (-0.5 * inv)
            t_m[p] = t0 * units[p] - (0.5 * inv) * c_m[p]
        tt = mat(t_m, [t_m[k] for k in range(n_obs)])
        for p in range(n_obs):
            dn_m[p] = inv * (tt[p] - (0.5 * n0) * (t_m[p] + t0 * units[p]))

        def half_step(n, z):
            t = 1.5 - 0.5 * n
            nc = mat(dn_m, [c_m[k] for k in range(n_obs)])
            for p in range(n_obs):
                t_m[p] = t * units[p] - 0.5 * nc[p]
            tz = mat(t_m, [dz_m[k] for k in range(n_obs)])
            for p in range(n_obs):
                dz_m[p] = tz[p] - (0.5 * z) * dn_m[p]
            return t

        def step(i, carry):
            n, z = carry
            t = half_step(n, z)
            tt = mat(t_m, [t_m[k] for k in range(n_obs)])
            for p in range(n_obs):
                q_m[p] = tt[p] - (0.5 * n) * (t_m[p] + t * units[p])
            dn = mat(dn_m, [q_m[k] for k in range(n_obs)])
            for p in range(n_obs):
                dn_m[p] = dn[p]
            return n * t * t, t * z
        n, z = lax.fori_loop(1, NS_STEPS - 1, step, (n0 * t0 * t0, t0))
        z = half_step(n, z) * z

        rs = 1.0 / jnp.sqrt(trace)
        scale = float((members - 1) ** 0.5) * rs
        alpha = scale * z

        def apply_z(x):
            return z * x + vec(dz_m, vec(c_m, x))
        h = apply_z(apply_z(gain)) * inv

        base = m_s[...]
        for p in range(n_obs):
            base = base + h[p:p + 1, :] * f_s[p]
        move = alpha * d_s[...]
        for q in range(n_obs):
            acc = None
            for p in range(n_obs):
                term = (scale * dz_m[q, p:p + 1, :]) * f_s[p]
                acc = term if acc is None else acc + term
            ft_s[q] = acc
            move = move + shift[q] * acc
        b_s[0] = base + move
        b_s[1] = base - move

        def updated(t, a):
            acc = b_s[a] + alpha * recv_c[t, a]
            for q in range(n_obs):
                acc = acc + v_s[t, a, q:q + 1, :] * ft_s[q]
            return acc

        @pl.when(cyc < cycles - 1)
        def _():
            for a in range(2):
                def back(g, carry):
                    for n in range(3):
                        tx, te, tl, t = pick(3 * g + n)
                        send_f[a, t] = updated(t, a)
                    for n in range(3):
                        tx, te, tl, t = pick(3 * g + n)
                        f_copy(a, tx, te, tl, me).start()
                    return carry
                lax.fori_loop(0, 5, back, 0)
                recv_f[a, me] = updated(me, a)

        @pl.when(cyc == cycles - 1)
        def _():
            def final(i, carry):
                te = (me_e + i) % 4
                for k in range(8):
                    new = updated(te * 4 + k // 2, k % 2)
                    for q in range(4):
                        out_s[te * 4 + q, pl.ds(k, 12, stride=8), :] = new[q * 12:(q + 1) * 12, :]
                for dz in (2, 1, 3, 0):
                    tz = (me_z + dz) % 4
                    own = jnp.logical_and(inside, jnp.logical_and(te == me_e, tz == me_z))

                    @pl.when(jnp.logical_not(own))
                    def _():
                        o_copy(te, tz, me).start()

                    @pl.when(own)
                    def _():
                        out_r[:, pl.ds(pl.multiple_of(me * 128, 128), 128)] = out_s[te * 4 + tz]
                return carry
            lax.fori_loop(0, 4, final, 0)

    def cycle(cyc, carry):
        def one(a, inner):
            forecast(cyc, a)
            return inner
        lax.fori_loop(0, 2, one, 0)
        analyse(cyc)
        return carry
    lax.fori_loop(0, cycles, cycle, 0)

    for a in range(2):
        c_all(a).wait_send()
        end_init(a)

    @pl.when(inside)
    def _():
        o_all(15).wait()

    @pl.when(jnp.logical_not(inside))
    def _():
        o_all(16).wait()
    out_ref[...] = out_r[...]


def solution(mesh):
    def local_step(ens_local, mix_op, w_in, w_out, obs_val, obs_prec, obs_idx, inflation):
        cycles, layers = obs_val.shape[0], w_in.shape[0]
        n_obs = obs_idx.shape[0]
        x0 = jnp.transpose(ens_local, (2, 0, 1)).reshape(96, 2048)
        u_t = jnp.transpose(w_out, (0, 2, 1))
        yobs = jnp.transpose(obs_val, (0, 2, 1))
        rinv = jnp.transpose(obs_prec)
        vmem = pl.BlockSpec(memory_space=pltpu.VMEM)
        smem = pl.BlockSpec(memory_space=pltpu.SMEM)
        dma = pltpu.SemaphoreType.DMA
        out = pl.pallas_call(
            functools.partial(kernel, (cycles, layers, n_obs)),
            out_shape=jax.ShapeDtypeStruct((96, 2048), F32),
            in_specs=[smem, smem, vmem, pl.BlockSpec(memory_space=pl.ANY), vmem, vmem, vmem, vmem],
            out_specs=vmem,
            scratch_shapes=[
                pltpu.VMEM((2048, 2048), BF16),
                pltpu.VMEM((2048, 2048), BF16),
                pltpu.VMEM((4, 2, layers, 48, 192), BF16),
                pltpu.VMEM((layers, 768, 128), BF16),
                pltpu.VMEM((layers, 48, 768), BF16),
                pltpu.VMEM((2, 4, 12, 2048), F32),
                pltpu.VMEM((2, 4, 12, 2048), F32),
                pltpu.VMEM((2, 2, 12, 2048), F32),
                pltpu.VMEM((cycles, n_obs, 128), F32),
                pltpu.VMEM((n_obs, 128), F32),
                pltpu.VMEM((2, 48, 2048), F32),
                pltpu.VMEM((48, 2048), BF16),
                pltpu.VMEM((128, 2048), BF16),
                pltpu.VMEM((16, 2, 48, 128), F32),
                pltpu.VMEM((2, 16, 48, 128), F32),
                pltpu.VMEM((2, 16, 48, 128), F32),
                pltpu.VMEM((16, 96, 128), F32),
                pltpu.VMEM((96, 2048), F32),
                pltpu.VMEM((16, 48, 128), F32),
                pltpu.VMEM((16, 2, n_obs, 128), F32),
                pltpu.VMEM((n_obs, 48, 128), F32),
                pltpu.VMEM((n_obs, 48, 128), F32),
                pltpu.VMEM((48, 128), F32),
                pltpu.VMEM((48, 128), F32),
                pltpu.VMEM((2, 48, 128), F32),
                pltpu.VMEM((n_obs, n_obs, 128), F32),
                pltpu.VMEM((n_obs, n_obs, 128), F32),
                pltpu.VMEM((n_obs, n_obs, 128), F32),
                pltpu.VMEM((n_obs, n_obs, 128), F32),
                pltpu.VMEM((n_obs, n_obs, 128), F32),
                dma(()),
                dma((layers, 4)), dma((layers, 4)), dma((layers, 4)), dma((layers, 4)),
                dma((4,)), dma((4,)), dma((2,)), dma((2,)),
                dma((2, 4)), dma((2, 4)), dma((2, 2)), dma((2, 2)),
                dma((2,)), dma((2,)),
                dma((2,)), dma((2,)),
                dma(()), dma(()),
            ],
            compiler_params=pltpu.CompilerParams(
                collective_id=0, has_side_effects=True, vmem_limit_bytes=60 * 1024 * 1024),
        )(obs_idx, inflation, x0, mix_op, w_in, u_t, yobs, rinv)
        return jnp.transpose(out.reshape(12, 8, 2048), (1, 2, 0))

    member_spec = P(("case", "ens"), None, "model")
    col_axes = ("case", "ens", "model")
    in_specs = (member_spec, P(None, None), P(None, None, "model"), P(None, "model", None), P(None, col_axes, None), P(col_axes, None), P(None), P(None))
    return jax.shard_map(local_step, mesh=mesh, in_specs=in_specs, out_specs=member_spec, check_vma=False)
```

```python
import functools

import jax
import jax.numpy as jnp
from jax import lax
from jax.experimental import pallas as pl
from jax.experimental.pallas import tpu as pltpu
from jax.sharding import PartitionSpec as P

NS_STEPS = 12
MESH_IDS = pl.DeviceIdType.MESH
F32 = jnp.float32
BF16 = jnp.bfloat16
C1 = 0.7978845608028654
C2 = 0.7978845608028654 * 0.044715


def gelu(x):
    th = jnp.tanh(x * (C1 + C2 * (x * x)))
    half = 0.5 * x
    return half + half * th


def kernel(dims, idx_ref, rho_ref, x0_ref, a_hbm, w_ref, u_ref, y_in, r_in, out_ref,
           a_v, at, wall, wt, ut, s0, r0, relay, y_ref, r_ref, hw, hb, mt, recv_c, recv_f, send_f, out_s, out_r,
           x_s, v_s, f_s, ft_s, m_s, d_s, b_s, c_m, dn_m, dz_m, t_m, q_m,
           sem_a, sem_zs, sem_wr, sem_hs, sem_vs, sem_ds, sem_dr, sem_bs, sem_br, sem_is, sem_ir, sem_rs, sem_rr,
           sem_cs, sem_cr, sem_fs, sem_fr, sem_os, sem_or):
    cycles, layers, n_obs = dims
    me_x = lax.axis_index("case")
    me_e = lax.axis_index("ens")
    me_z = lax.axis_index("model")
    grp = me_z // 2
    low = me_z % 2
    core = me_e % 2
    far = 1 - me_x
    mate = me_e + 1 - 2 * core
    me = me_e * 4 + me_x * 2 + low
    inside = grp == me_x
    members = 32

    def ids(tx, te, tz):
        return {"case": tx, "ens": te, "model": tz}

    def send(src, dst, ssem, rsem, dev):
        return pltpu.make_async_remote_copy(
            src_ref=src, dst_ref=dst, send_sem=ssem, recv_sem=rsem, device_id=dev, device_id_type=MESH_IDS)

    bar = pltpu.get_barrier_semaphore()
    for dx in range(2):
        for de in range(4):
            for dz in range(4):
                if (dx, de, dz) != (0, 0, 0):
                    pl.semaphore_signal(bar, inc=1, device_id=ids((me_x + dx) % 2, (me_e + de) % 4, (me_z + dz) % 4), device_id_type=MESH_IDS)
    copy_a = pltpu.make_async_copy(a_hbm, a_v, sem_a)
    copy_a.start()
    for j in range(16):
        out_s[j] = x0_ref[:, j * 128:(j + 1) * 128]
        for a in range(2):
            for i in range(4):
                s0[a, i, :, j * 128:(j + 1) * 128] = out_s[j, pl.ds(2 * i + a, 12, stride=8), :]
    wall[me_z, 0] = w_ref[...]
    wall[me_z, 1] = u_ref[...]
    pl.semaphore_wait(bar, 31)

    def i_copy(a, i):
        return send(s0.at[a, i], r0.at[a, me_z], sem_is.at[a, i], sem_ir.at[a, me_z], ids(i // 2, me_e, 2 * me_x + i % 2))

    def i_arrive(a, m):
        return send(s0.at[a, 0], r0.at[a, m], sem_is.at[a, 0], sem_ir.at[a, m], ids(far, me_e, me_z))

    def x_copy(a, k):
        i = 2 * far + k
        return send(s0.at[a, i], relay.at[a, k], sem_is.at[a, i], sem_rr.at[a, k], ids(far, me_e, me_z))

    def r_copy(a, k):
        return send(relay.at[a, k], r0.at[a, me_z], sem_rs.at[a, k], sem_ir.at[a, me_z], ids(me_x, me_e, 2 * far + k))

    def b_copy(n):
        dev = ids(me_z // 2, me_e, 2 * me_x + low)
        return send(y_in, y_ref, sem_bs.at[0], sem_br.at[0], dev) if n == 0 else send(r_in, r_ref, sem_bs.at[1], sem_br.at[1], dev)

    def home(l):
        return me_x == l % 2, me_e // 2 == (l // 2) % 2

    def z_copy(l, dz, slot):
        tz = (me_z + dz) % 4
        return send(wall.at[me_z, core, l], wall.at[slot, core, l], sem_zs.at[l, tz], sem_wr.at[l, slot], ids(me_x, me_e, tz))

    def h_copy(l, q):
        return send(wall.at[q, core, l], wall.at[q, core, l], sem_hs.at[l, q], sem_wr.at[l, q], ids(far, me_e, me_z))

    def v_copy(l, q):
        return send(wall.at[q, core, l], wall.at[q, core, l], sem_vs.at[l, q], sem_wr.at[l, q], ids(me_x, (me_e + 2) % 4, me_z))

    def d_copy(q, c):
        return send(wall.at[q, c], wall.at[q, c], sem_ds.at[q], sem_dr.at[q], ids(me_x, mate, me_z))

    shifts = (2, 1, 3)

    def w_stage(stage):
        for l in range(layers):
            on_x, on_y = home(l)
            away = jnp.logical_not(on_x)
            off = jnp.logical_not(on_y)
            first = jnp.logical_and(on_x, on_y)
            second = jnp.logical_and(away, on_y)
            if stage == 0:
                @pl.when(first)
                def _():
                    for dz in shifts:
                        z_copy(l, dz, me_z).start()
            if stage == 1:
                @pl.when(first)
                def _():
                    for dz in shifts:
                        q = (me_z + dz) % 4
                        z_copy(l, dz, q).wait()
                        h_copy(l, q).start()
                        v_copy(l, q).start()
            if stage == 2:
                @pl.when(second)
                def _():
                    for dz in shifts:
                        q = (me_z + dz) % 4
                        h_copy(l, q).wait_recv()
                        v_copy(l, q).start()
            if stage == 3:
                @pl.when(off)
                def _():
                    for dz in shifts:
                        v_copy(l, (me_z + dz) % 4).wait_recv()

                @pl.when(first)
                def _():
                    for dz in shifts:
                        h_copy(l, (me_z + dz) % 4).wait_send()

                @pl.when(on_y)
                def _():
                    for dz in shifts:
                        v_copy(l, (me_z + dz) % 4).wait_send()
        if stage == 3:
            for dz in shifts:
                d_copy((me_z + dz) % 4, core).start()
            for dz in shifts:
                q = (me_z + dz) % 4
                d_copy(q, core).wait_send()
                d_copy(q, 1 - core).wait_recv()

    def start_init(a):
        @pl.when(inside)
        def _():
            for i in range(4):
                @pl.when(me_z != i)
                def _():
                    i_copy(a, i).start()
            r0[a, me_z] = s0[a, me_z]

        @pl.when(jnp.logical_not(inside))
        def _():
            for k in range(2):
                x_copy(a, k).start()
            for k in range(2):
                i_copy(a, 2 * me_x + k).start()

    def start_relay(a):
        @pl.when(inside)
        def _():
            for k in range(2):
                x_copy(a, k).wait_recv()
                r_copy(a, k).start()

    def end_init(a):
        @pl.when(inside)
        def _():
            for i in range(4):
                @pl.when(me_z != i)
                def _():
                    i_copy(a, i).wait_send()
            for k in range(2):
                r_copy(a, k).wait_send()

        @pl.when(jnp.logical_not(inside))
        def _():
            for k in range(2):
                x_copy(a, k).wait_send()
                i_copy(a, 2 * me_x + k).wait_send()

    w_stage(0)
    start_init(0)

    @pl.when(inside)
    def _():
        y_ref[...] = y_in[...]
        r_ref[...] = r_in[...]

    @pl.when(jnp.logical_not(inside))
    def _():
        b_copy(0).start()
        b_copy(1).start()
    mt[48:128, :] = jnp.zeros((80, 2048), BF16)

    copy_a.wait()
    row = lax.broadcasted_iota(jnp.int32, (256, 256), 0)
    col = lax.broadcasted_iota(jnp.int32, (256, 256), 1)
    eye = jnp.where(row == col, 1.0, 0.0).astype(BF16)

    def flip(i, carry):
        for j in range(8):
            tile = a_v[pl.ds(pl.multiple_of(i * 256, 256), 256), j * 256:(j + 1) * 256]
            at[j * 256:(j + 1) * 256, pl.ds(pl.multiple_of(i * 256, 256), 256)] = lax.dot_general(
                eye, tile, (((1,), (1,)), ((), ())), preferred_element_type=F32).astype(BF16)
        return carry

    w_stage(1)
    start_relay(0)
    w_stage(2)
    start_init(1)
    lax.fori_loop(0, 8, flip, 0)
    w_stage(3)
    start_relay(1)

    for l in range(layers):
        parts = [wall[q, 0, l].astype(F32) for q in range(4)]
        full = jnp.concatenate([jnp.concatenate(parts, axis=1), jnp.zeros((80, 768), F32)], axis=0)
        wt[l] = jnp.transpose(full).astype(BF16)
        ut[l] = jnp.concatenate([wall[q, 1, l].astype(F32) for q in range(4)], axis=1).astype(BF16)

    @pl.when(jnp.logical_not(inside))
    def _():
        b_copy(0).wait()
        b_copy(1).wait()

    def spot(b):
        tx = (me_x + (7 - b) // 4) % 2
        te = 2 * ((me_e // 2 + (7 - b) // 2) % 2) + (core + 7 - b) % 2
        return tx, te

    def pick(i):
        tx, te = spot(i // 2)
        tl = (low + i + 1) % 2
        return tx, te, tl, te * 4 + tx * 2 + tl

    def c_copy(a, tx, te, tl, slot):
        t = te * 4 + tx * 2 + tl
        return send(hw.at[a, :, pl.ds(pl.multiple_of(t * 128, 128), 128)], recv_c.at[slot, a],
                    sem_cs.at[a], sem_cr.at[a], ids(tx, te, 2 * grp + tl))

    def f_copy(a, tx, te, tl, slot):
        t = te * 4 + tx * 2 + tl
        return send(send_f.at[a, t], recv_f.at[a, slot], sem_fs.at[a], sem_fr.at[a], ids(tx, te, 2 * grp + tl))

    def o_copy(te, tz, slot):
        t = te * 4 + tz
        return send(out_s.at[t], out_r.at[:, pl.ds(pl.multiple_of(slot * 128, 128), 128)],
                    sem_os, sem_or, ids(grp, te, tz))

    def c_all(a):
        return send(recv_c.at[0:15, a], recv_c.at[0:15, a], sem_cs.at[a], sem_cr.at[a], ids(far, me_e, me_z))

    def f_all(a):
        return send(send_f.at[a, 0:15], recv_f.at[a, 0:15], sem_fs.at[a], sem_fr.at[a], ids(far, me_e, me_z))

    def o_all(n):
        return send(out_s.at[0:n], out_s.at[0:n], sem_os, sem_or, ids(far, me_e, me_z))

    def forecast(cyc, a):
        @pl.when(cyc == 0)
        def _():
            for q in range(4):
                @pl.when(jnp.logical_not(jnp.logical_and(inside, me_z == q)))
                def _():
                    i_arrive(a, q).wait_recv()
            for q in range(4):
                hw[a, q * 12:(q + 1) * 12, :] = r0[a, q]
            hb[...] = hw[a].astype(BF16)

        @pl.when(cyc > 0)
        def _():
            c_all(a).wait_send()
            f_all(a).wait()
            for j in range(16):
                sl = slice(j * 128, (j + 1) * 128)
                block = recv_f[a, j]
                hw[a, :, sl] = block
                hb[:, sl] = block.astype(BF16)

        def mix_all():
            for n in range(2):
                sl = slice(n * 1024, (n + 1) * 1024)
                mt[0:48, sl] = jnp.dot(hb[...], at[:, sl], preferred_element_type=F32).astype(BF16)

        def tile(l, sl):
            mix = mt[:, sl]
            parts = []
            for n in range(6):
                hid = jnp.dot(wt[l, n * 128:(n + 1) * 128, :], mix, preferred_element_type=F32)
                parts.append(gelu(hid).astype(BF16))
            upd = jnp.dot(ut[l], jnp.concatenate(parts, axis=0), preferred_element_type=F32)
            new = hw[a, :, sl] + upd
            hw[a, :, sl] = new
            return new

        def layer(l, carry):
            mix_all()
            for b in range(8):
                sl = slice(b * 256, (b + 1) * 256)
                hb[:, sl] = tile(l, sl).astype(BF16)
            return carry
        lax.fori_loop(0, layers - 1, layer, 0)

        def sends(b):
            tx, te = spot(b)
            for tl in ((1 - low, low) if b < 7 else (1 - low,)):
                c_copy(a, tx, te, tl, me).start()

        mix_all()
        for b in range(8):
            tx, te = spot(b)
            tile(layers - 1, pl.ds(pl.multiple_of((2 * te + tx) * 256, 256), 256))
            if b in (4, 7):
                for n in (range(5) if b == 4 else range(5, 8)):
                    sends(n)
        recv_c[me, a] = hw[a, :, pl.ds(pl.multiple_of(me * 128, 128), 128)]

    def mat(p_ref, rows):
        out = []
        for i in range(n_obs):
            acc = None
            for k in range(n_obs):
                term = p_ref[i, k:k + 1, :] * rows[k]
                acc = term if acc is None else acc + term
            out.append(acc)
        return out

    def vec(p_ref, x):
        acc = None
        for k in range(n_obs):
            term = x[k:k + 1, :] * p_ref[k]
            acc = term if acc is None else acc + term
        return acc

    sub = lax.broadcasted_iota(jnp.int32, (n_obs, 128), 0)
    units = [jnp.where(sub == i, 1.0, 0.0).astype(F32) for i in range(n_obs)]
    c0 = (members - 1) / rho_ref[0]

    def analyse(cyc):
        root = jnp.sqrt(r_ref[...])
        means = []
        for a in range(2):
            c_all(a).wait_recv()

            def add(j, acc):
                return acc + ((recv_c[4 * j, a] + recv_c[4 * j + 1, a]) + (recv_c[4 * j + 2, a] + recv_c[4 * j + 3, a]))
            part = lax.fori_loop(0, 4, add, jnp.zeros((48, 128), F32)) * (2.0 / members)
            means.append(part)

            def centre(j, carry):
                for n in range(4):
                    block = recv_c[4 * j + n, a] - part
                    recv_c[4 * j + n, a] = block
                    x_s[4 * j + n] = block
                return carry
            lax.fori_loop(0, 4, centre, 0)

            for p in range(n_obs):
                ip = idx_ref[p]
                v_s[:, a, p:p + 1, :] = x_s[:, pl.ds(ip, 1), :] * root[p:p + 1, :]

            for base_p in range(0, n_obs, 6):
                def outer(j, accs):
                    accs = list(accs)
                    for n in range(2):
                        x = recv_c[2 * j + n, a]
                        for p in range(6):
                            accs[p] = accs[p] + v_s[2 * j + n, a, base_p + p:base_p + p + 1, :] * x
                    return tuple(accs)
                start = tuple(jnp.zeros((48, 128), F32) if a == 0 else f_s[base_p + p] for p in range(6))
                sums = lax.fori_loop(0, 8, outer, start)
                for p in range(6):
                    f_s[base_p + p] = sums[p]

        mean = 0.5 * (means[0] + means[1])
        delta = 0.5 * (means[0] - means[1])
        m_s[...] = mean
        d_s[...] = delta
        shift = [root[p:p + 1, :] * d_s[pl.ds(idx_ref[p], 1), :] for p in range(n_obs)]
        for p in range(n_obs):
            f_s[p] = f_s[p] + (float(members) * shift[p]) * delta

        gain = []
        for q in range(n_obs):
            iq = idx_ref[q]
            c_m[:, q:q + 1, :] = f_s[:, pl.ds(iq, 1), :] * root[q:q + 1, :]
            gain.append(root[q:q + 1, :] * (y_ref[cyc, q:q + 1, :] - m_s[pl.ds(iq, 1), :]))
        gain = jnp.concatenate(gain, axis=0)

        trace = None
        for p in range(n_obs):
            term = c_m[p, p:p + 1, :]
            trace = term if trace is None else trace + term
        trace = trace + members * c0
        inv = 1.0 / trace
        n0 = c0 * inv
        t0 = 1.5 - 0.5 * n0
        for p in range(n_obs):
            dz_m[p] = units[p] * (-0.5 * inv)
            t_m[p] = t0 * units[p] - (0.5 * inv) * c_m[p]
        tt = mat(t_m, [t_m[k] for k in range(n_obs)])
        for p in range(n_obs):
            dn_m[p] = inv * (tt[p] - (0.5 * n0) * (t_m[p] + t0 * units[p]))

        def half_step(n, z):
            t = 1.5 - 0.5 * n
            nc = mat(dn_m, [c_m[k] for k in range(n_obs)])
            for p in range(n_obs):
                t_m[p] = t * units[p] - 0.5 * nc[p]
            tz = mat(t_m, [dz_m[k] for k in range(n_obs)])
            for p in range(n_obs):
                dz_m[p] = tz[p] - (0.5 * z) * dn_m[p]
            return t

        def step(i, carry):
            n, z = carry
            t = half_step(n, z)
            tt = mat(t_m, [t_m[k] for k in range(n_obs)])
            for p in range(n_obs):
                q_m[p] = tt[p] - (0.5 * n) * (t_m[p] + t * units[p])
            dn = mat(dn_m, [q_m[k] for k in range(n_obs)])
            for p in range(n_obs):
                dn_m[p] = dn[p]
            return n * t * t, t * z
        n, z = lax.fori_loop(1, NS_STEPS - 1, step, (n0 * t0 * t0, t0))
        z = half_step(n, z) * z

        rs = 1.0 / jnp.sqrt(trace)
        scale = float((members - 1) ** 0.5) * rs
        alpha = scale * z

        def apply_z(x):
            return z * x + vec(dz_m, vec(c_m, x))
        h = apply_z(apply_z(gain)) * inv

        base = m_s[...]
        for p in range(n_obs):
            base = base + h[p:p + 1, :] * f_s[p]
        move = alpha * d_s[...]
        for q in range(n_obs):
            acc = None
            for p in range(n_obs):
                term = (scale * dz_m[q, p:p + 1, :]) * f_s[p]
                acc = term if acc is None else acc + term
            ft_s[q] = acc
            move = move + shift[q] * acc
        b_s[0] = base + move
        b_s[1] = base - move

        def updated(t, a):
            acc = b_s[a] + alpha * recv_c[t, a]
            for q in range(n_obs):
                acc = acc + v_s[t, a, q:q + 1, :] * ft_s[q]
            return acc

        @pl.when(cyc < cycles - 1)
        def _():
            for a in range(2):
                def back(g, carry):
                    for n in range(3):
                        tx, te, tl, t = pick(3 * g + n)
                        send_f[a, t] = updated(t, a)
                    for n in range(3):
                        tx, te, tl, t = pick(3 * g + n)
                        f_copy(a, tx, te, tl, me).start()
                    return carry
                lax.fori_loop(0, 5, back, 0)
                recv_f[a, me] = updated(me, a)

        @pl.when(cyc == cycles - 1)
        def _():
            def final(i, carry):
                te = (me_e + i) % 4
                for k in range(8):
                    new = updated(te * 4 + k // 2, k % 2)
                    for q in range(4):
                        out_s[te * 4 + q, pl.ds(k, 12, stride=8), :] = new[q * 12:(q + 1) * 12, :]
                for dz in (2, 1, 3, 0):
                    tz = (me_z + dz) % 4
                    own = jnp.logical_and(inside, jnp.logical_and(te == me_e, tz == me_z))

                    @pl.when(jnp.logical_not(own))
                    def _():
                        o_copy(te, tz, me).start()

                    @pl.when(own)
                    def _():
                        out_r[:, pl.ds(pl.multiple_of(me * 128, 128), 128)] = out_s[te * 4 + tz]
                return carry
            lax.fori_loop(0, 4, final, 0)

    def cycle(cyc, carry):
        def one(a, inner):
            forecast(cyc, a)
            return inner
        lax.fori_loop(0, 2, one, 0)
        analyse(cyc)
        return carry
    lax.fori_loop(0, cycles, cycle, 0)

    for a in range(2):
        c_all(a).wait_send()
        end_init(a)

    @pl.when(inside)
    def _():
        o_all(15).wait()

    @pl.when(jnp.logical_not(inside))
    def _():
        o_all(16).wait()
    out_ref[...] = out_r[...]


def solution(mesh):
    def local_step(ens_local, mix_op, w_in, w_out, obs_val, obs_prec, obs_idx, inflation):
        cycles, layers = obs_val.shape[0], w_in.shape[0]
        n_obs = obs_idx.shape[0]
        x0 = jnp.transpose(ens_local, (2, 0, 1)).reshape(96, 2048)
        u_t = jnp.transpose(w_out, (0, 2, 1))
        yobs = jnp.transpose(obs_val, (0, 2, 1))
        rinv = jnp.transpose(obs_prec)
        vmem = pl.BlockSpec(memory_space=pltpu.VMEM)
        smem = pl.BlockSpec(memory_space=pltpu.SMEM)
        dma = pltpu.SemaphoreType.DMA
        out = pl.pallas_call(
            functools.partial(kernel, (cycles, layers, n_obs)),
            out_shape=jax.ShapeDtypeStruct((96, 2048), F32),
            in_specs=[smem, smem, vmem, pl.BlockSpec(memory_space=pl.ANY), vmem, vmem, vmem, vmem],
            out_specs=vmem,
            scratch_shapes=[
                pltpu.VMEM((2048, 2048), BF16),
                pltpu.VMEM((2048, 2048), BF16),
                pltpu.VMEM((4, 2, layers, 48, 192), BF16),
                pltpu.VMEM((layers, 768, 128), BF16),
                pltpu.VMEM((layers, 48, 768), BF16),
                pltpu.VMEM((2, 4, 12, 2048), F32),
                pltpu.VMEM((2, 4, 12, 2048), F32),
                pltpu.VMEM((2, 2, 12, 2048), F32),
                pltpu.VMEM((cycles, n_obs, 128), F32),
                pltpu.VMEM((n_obs, 128), F32),
                pltpu.VMEM((2, 48, 2048), F32),
                pltpu.VMEM((48, 2048), BF16),
                pltpu.VMEM((128, 2048), BF16),
                pltpu.VMEM((16, 2, 48, 128), F32),
                pltpu.VMEM((2, 16, 48, 128), F32),
                pltpu.VMEM((2, 16, 48, 128), F32),
                pltpu.VMEM((16, 96, 128), F32),
                pltpu.VMEM((96, 2048), F32),
                pltpu.VMEM((16, 48, 128), F32),
                pltpu.VMEM((16, 2, n_obs, 128), F32),
                pltpu.VMEM((n_obs, 48, 128), F32),
                pltpu.VMEM((n_obs, 48, 128), F32),
                pltpu.VMEM((48, 128), F32),
                pltpu.VMEM((48, 128), F32),
                pltpu.VMEM((2, 48, 128), F32),
                pltpu.VMEM((n_obs, n_obs, 128), F32),
                pltpu.VMEM((n_obs, n_obs, 128), F32),
                pltpu.VMEM((n_obs, n_obs, 128), F32),
                pltpu.VMEM((n_obs, n_obs, 128), F32),
                pltpu.VMEM((n_obs, n_obs, 128), F32),
                dma(()),
                dma((layers, 4)), dma((layers, 4)), dma((layers, 4)), dma((layers, 4)),
                dma((4,)), dma((4,)), dma((2,)), dma((2,)),
                dma((2, 4)), dma((2, 4)), dma((2, 2)), dma((2, 2)),
                dma((2,)), dma((2,)),
                dma((2,)), dma((2,)),
                dma(()), dma(()),
            ],
            compiler_params=pltpu.CompilerParams(
                collective_id=0, has_side_effects=True, vmem_limit_bytes=60 * 1024 * 1024),
        )(obs_idx, inflation, x0, mix_op, w_in, u_t, yobs, rinv)
        return jnp.transpose(out.reshape(12, 8, 2048), (1, 2, 0))

    member_spec = P(("case", "ens"), None, "model")
    col_axes = ("case", "ens", "model")
    in_specs = (member_spec, P(None, None), P(None, None, "model"), P(None, "model", None), P(None, col_axes, None), P(col_axes, None), P(None), P(None))
    return jax.shard_map(local_step, mesh=mesh, in_specs=in_specs, out_specs=member_spec, check_vma=False)
```
